16 devices in a mesh: dp: 2 (over y, z), tp: 8 (over x, core).
Axes of the slice: x: 4, y: 2, z: 1, core: 2. Of those that a mesh axis runs over, the one named last changes fastest.
The devices are a block of a 4x4x8 slice.
Arguments:
- x: bfloat16 [4096, 2048], P('dp'), parts along dimension 0
- dy: bfloat16 [4096, 2048], P('dp'), parts along dimension 0
- gate: bfloat16 [4096, 5120], P('dp', 'tp'), parts along dimension 0
- up: bfloat16 [4096, 5120], P('dp', 'tp'), parts along dimension 0
- w_gate: bfloat16 [2048, 5120], P(None, 'tp')
- w_up: bfloat16 [2048, 5120], P(None, 'tp')
- w_down: bfloat16 [5120, 2048], P('tp')
Outputs:
- output 1: bfloat16 [4096, 2048], P('dp'), parts along dimension 0
- output 2: bfloat16 [4096, 5120], P('dp', 'tp'), parts along dimension 0
- output 3: bfloat16 [4096, 5120], P('dp', 'tp'), parts along dimension 0
- output 4: bfloat16 [10240, 2048], P(('dp', 'tp')), parts along dimension 0
There are 2 independent parts. The reference program is written for one: setup_inputs(seed, part) draws one part's arguments, and reference() takes and returns one part's arrays. A program takes and returns all parts, laid end to end along the dimension named above; an argument that names none is the same for every part.
All inputs are finite; a program needn't handle non-finite values.
Results may differ from the reference program's by a relative error of at most 0.012.
Values are sent between devices in bfloat16 or wider.
A program may use at most 768 MiB of HBM per device.

```python
import jax
import jax.numpy as jnp

ROWS = 2048
D = 2048
FF = 5120


def act(gate, up):
    return jax.nn.gelu(gate) * up


def setup_inputs(seed: int = 0, part: int = 0) -> dict:
    kx, ky, ka, kb, kg, ku, kd = jax.random.split(jax.random.key(seed), 7)
    kx, ky, ka, kb = (jax.random.fold_in(k, part) for k in (kx, ky, ka, kb))
    drawn = {
        "x": jax.random.normal(kx, (ROWS, D), jnp.float32),
        "dy": jax.random.normal(ky, (ROWS, D), jnp.float32),
        "gate": jax.random.normal(ka, (ROWS, FF), jnp.float32),
        "up": jax.random.normal(kb, (ROWS, FF), jnp.float32),
        "w_gate": jax.random.normal(kg, (D, FF), jnp.float32) * D**-0.5,
        "w_up": jax.random.normal(ku, (D, FF), jnp.float32) * D**-0.5,
        "w_down": jax.random.normal(kd, (FF, D), jnp.float32) * FF**-0.5,
    }
    return {k: v.astype(jnp.bfloat16) for k, v in drawn.items()}


def reference(x, dy, gate, up, w_gate, w_up, w_down):
    hidden, back = jax.vjp(act, gate.astype(jnp.float32), up.astype(jnp.float32))
    d_hidden = jnp.dot(dy, w_down.T, preferred_element_type=jnp.float32)
    d_gate, d_up = (g.astype(jnp.bfloat16) for g in back(d_hidden))
    dx = jnp.dot(d_gate, w_gate.T, preferred_element_type=jnp.float32) + jnp.dot(d_up, w_up.T, preferred_element_type=jnp.float32)
    dw_gate = jnp.dot(x.T, d_gate, preferred_element_type=jnp.float32)
    dw_up = jnp.dot(x.T, d_up, preferred_element_type=jnp.float32)
    dw_down = jnp.dot(hidden.astype(jnp.bfloat16).T, dy, preferred_element_type=jnp.float32)
    return tuple(g.astype(jnp.bfloat16) for g in (dx, dw_gate, dw_up, dw_down))
```

```python
import functools

import jax
import jax.numpy as jnp
from jax import lax
from jax.experimental import pallas as pl
from jax.experimental.pallas import tpu as pltpu
from jax.sharding import PartitionSpec as P

MESH = pl.DeviceIdType.MESH
CHIPS = 4
BLOCK = 256
PART = BLOCK // 2
STRIP = 32
TILE = 256


def act(gate, up):
    return jax.nn.gelu(gate) * up


def dot(a, b, contract):
    return lax.dot_general(a, b, ((contract[:1], contract[1:]), ((), ())), preferred_element_type=jnp.float32)


def main_kernel(
    x_hbm, dy_hbm, gate_hbm, up_hbm, wg_hbm, wu_hbm, wd_hbm,
    dx, dw, dwd,
    x, dy, gu, w, wd, hid, hid_t, dh, own, stage, sendbuf, far, near,
    in_sem, row_sem, term_send, term_recv, rs_send, far_recv, near_recv,
    ag_send, ag_recv, fwd_send, fwd_recv, peer_send, peer_recv,
):
    tokens, d = x.shape
    f = wd.shape[0]
    half = d // 2
    chunk_rows = tokens // CHIPS
    me = lax.axis_index("tp")
    chip, core = lax.div(me, 2), lax.rem(me, 2)
    peer = chip * 2 + 1 - core
    mine = pl.ds(pl.multiple_of(core * half, half), half)
    theirs = pl.ds(pl.multiple_of((1 - core) * half, half), half)

    def chip_at(step):
        return lax.rem(chip + step, CHIPS)

    def device_at(step):
        return chip_at(step) * 2 + core

    steps = (1, CHIPS - 1)

    barrier = pltpu.get_barrier_semaphore()
    for other in (device_at(1), device_at(CHIPS - 1), peer):
        pl.semaphore_signal(barrier, inc=1, device_id={"tp": other}, device_id_type=MESH)

    def remote(src, dst, send, recv, device):
        return pltpu.make_async_remote_copy(
            src_ref=src, dst_ref=dst, send_sem=send, recv_sem=recv, device_id={"tp": device}, device_id_type=MESH
        )

    def row_at(step, i, p=0):
        return pl.multiple_of(chip_at(step) * chunk_rows + i * BLOCK + p * PART, PART)

    def row_copies(b, step, i):
        r = pl.ds(row_at(step, i), BLOCK)
        return (
            pltpu.make_async_copy(dy_hbm.at[r], dy.at[r], row_sem.at[0, b]),
            pltpu.make_async_copy(gate_hbm.at[r], gu.at[r, pl.ds(0, f)], row_sem.at[1, b]),
            pltpu.make_async_copy(up_hbm.at[r], gu.at[r, pl.ds(f, f)], row_sem.at[2, b]),
        )

    def start_rows(b, step, i):
        for c in row_copies(b, step, i):
            c.start()

    def x_copy(b):
        r = pl.ds(pl.multiple_of(b * BLOCK, BLOCK), BLOCK)
        return pltpu.make_async_copy(x_hbm.at[r], x.at[r], row_sem.at[3, b])

    in_wd = pltpu.make_async_copy(wd_hbm, wd, in_sem.at[0])
    in_wg = pltpu.make_async_copy(wg_hbm, w.at[:, pl.ds(0, f)], in_sem.at[1])
    in_wu = pltpu.make_async_copy(wu_hbm, w.at[:, pl.ds(f, f)], in_sem.at[2])
    in_wd.start()
    start_rows(0, 2, 0)
    in_wg.start()
    in_wu.start()
    start_rows(1, 2, 1)

    def hidden_block(b, step, i):
        start = row_at(step, i)
        for c in row_copies(b, step, i):
            c.wait()
        dh[...] = dot(dy[pl.ds(start, BLOCK), :], wd[...], (1, 1))

        @pl.loop(0, BLOCK // STRIP)
        def _(s):
            here = pl.ds(pl.multiple_of(s * STRIP, STRIP), STRIP)
            r = pl.ds(pl.multiple_of(start + s * STRIP, STRIP), STRIP)
            h, back = jax.vjp(act, gu[r, pl.ds(0, f)].astype(jnp.float32), gu[r, pl.ds(f, f)].astype(jnp.float32))
            d_gate, d_up = back(dh[here, :])
            gu[r, pl.ds(0, f)] = d_gate.astype(gu.dtype)
            gu[r, pl.ds(f, f)] = d_up.astype(gu.dtype)
            hid[here, :] = h.astype(hid.dtype)

        hid_t[:, pl.ds(pl.multiple_of(start, BLOCK), BLOCK)] = hid[...].T

    def term_copy(b, step, i, slot):
        rows = pl.ds(row_at(step, i), BLOCK)
        return remote(stage.at[slot], dx.at[rows, theirs], term_send.at[slot], term_recv.at[b], peer)

    def term_block(b, step, i, slot):
        rows = pl.ds(row_at(step, i), BLOCK)
        width = half // 2
        for q in range(2):
            cols = pl.ds(pl.multiple_of((1 - core) * half + q * width, width), width)
            stage[slot, :, q * width : (q + 1) * width] = dot(gu[rows, :], w[cols, :], (1, 1)).astype(stage.dtype)
        term_copy(b, step, i, slot).start()
        for q in range(2):
            cols = pl.ds(pl.multiple_of(core * half + q * width, width), width)
            own[:, q * width : (q + 1) * width] = dot(gu[rows, :], w[cols, :], (1, 1))
        term_copy(b, step, i, slot).wait_recv()

    def summed(step, i, p):
        r = pl.ds(row_at(step, i, p), PART)
        return own[pl.ds(pl.multiple_of(p * PART, PART), PART), :] + dx[r, mine].astype(jnp.float32)

    def far_copy(i, side):
        return remote(
            sendbuf.at[i, side], far.at[side, i], rs_send.at[i, side], far_recv.at[side, i], device_at(steps[side])
        )

    def near_copy(j, i, p, side, step):
        return remote(
            sendbuf.at[2 + j, p], near.at[side, i, p], rs_send.at[2 + j, p], near_recv.at[side, i, p], device_at(step)
        )

    in_wd.wait()

    @pl.loop(0, 2)
    def _(i):
        hidden_block(i, 2, i)
        start_rows(2 + i, 1 + 2 * i, 0)
        x_copy(i).start()

        @pl.when(i == 0)
        def _():
            in_wg.wait()
            in_wu.wait()
            pl.semaphore_wait(barrier, 3)

        term_block(i, 2, i, i)
        for p in range(2):
            sendbuf[i, p] = summed(2, i, p).astype(sendbuf.dtype)
            far_copy(i, p).start()

    @pl.loop(0, 4)
    def _(j):
        side, i = lax.rem(j, 2), lax.div(j, 2)
        step = 1 + 2 * side
        hidden_block(2 + j, step, i)

        @pl.when(j < 2)
        def _():
            start_rows(4 + j, step, 1)

        @pl.when(j >= 2)
        def _():
            start_rows(4 + j, 0, side)

        x_copy(2 + j).start()
        term_copy(0, step, i, side).wait_send()
        term_block(2 + j, step, i, side)
        plain = 1 - side
        sendbuf[2 + j, plain] = summed(step, i, plain).astype(sendbuf.dtype)
        near_copy(j, i, plain, side, step).start()
        remote(sendbuf.at[0, 0], far.at[side, i], rs_send.at[0, 0], far_recv.at[side, i], peer).wait_recv()
        sendbuf[2 + j, side] = (summed(step, i, side) + far[side, i].astype(jnp.float32)).astype(sendbuf.dtype)
        near_copy(j, i, side, side, step).start()

    for i in range(2):
        hidden_block(6 + i, 0, i)
        x_copy(6 + i).start()

    @pl.loop(0, 4)
    def _(t):
        cols = pl.ds(pl.multiple_of(t * (d // 4), d // 4), d // 4)
        dwd[:, cols] = dot(hid_t[...], dy[:, cols], (1, 0)).astype(dwd.dtype)

    def direct(i, p, side):
        r = pl.ds(row_at(0, i, p), PART)
        return remote(
            dx.at[r, mine], dx.at[r, mine], ag_send.at[side, i, p], ag_recv.at[side, i, p], device_at(steps[side])
        )

    def forward(i, side):
        r = pl.ds(row_at(steps[1 - side], i, side), PART)
        return remote(dx.at[r, mine], dx.at[r, mine], fwd_send.at[side, i], fwd_recv.at[side, i], device_at(steps[side]))

    peers = []

    def share(step, i, p, rows=PART):
        k, r = len(peers), pl.ds(row_at(step, i, p), rows)
        peers.append(remote(dx.at[r, mine], dx.at[r, mine], peer_send.at[k], peer_recv.at[k], peer))
        peers[-1].start()

    def own_block(i):
        term_copy(0, 0, i, i).wait_send()
        term_block(6 + i, 0, i, i)
        for p in range(2):
            for side in range(2):
                near_copy(0, i, p, side, 0).wait_recv()
            total = summed(0, i, p)
            for side in range(2):
                total += near[side, i, p].astype(jnp.float32)
            dx[pl.ds(row_at(0, i, p), PART), mine] = total.astype(dx.dtype)
            direct(i, p, p).start()
        direct(i, 1, 0).start()
        direct(i, 0, 1).start()
        share(0, i, 0, BLOCK)

    def weight_tiles(lo, hi):
        @pl.loop(lo, hi)
        def _(t):
            cols = pl.ds(pl.multiple_of(t * TILE, TILE), TILE)
            dw[cols, :] = dot(x[:, cols], gu[...], (0, 0)).astype(dw.dtype)

    def relay(i):
        for side in range(2):
            direct(i, side, side).wait_recv()
            forward(i, side).start()
            share(steps[1 - side], i, side)

    def keep(i):
        for side in range(2):
            direct(i, 1 - side, side).wait_recv()
            share(steps[1 - side], i, 1 - side)

    def last(i):
        for side in range(2):
            forward(i, side).wait_recv()
            share(2, i, side)

    own_block(0)
    for b in range(8):
        x_copy(b).wait()
    weight_tiles(0, 2)
    own_block(1)
    weight_tiles(2, 4)
    relay(0)
    weight_tiles(4, 5)
    keep(0)
    weight_tiles(5, 7)
    relay(1)
    weight_tiles(7, d // TILE)
    keep(1)
    last(0)
    last(1)

    for i in range(2):
        term_copy(0, 0, i, i).wait_send()
        for p in range(2):
            far_copy(i, p).wait_send()
            for side in range(2):
                near_copy(2 * i + side, i, p, side, steps[side]).wait_send()
                direct(i, p, side).wait_send()
        for side in range(2):
            forward(i, side).wait_send()
    for c in peers:
        c.wait()


def write_kernel(dx, dw, dwd, dx_hbm, dwg_hbm, dwu_hbm, dwd_hbm, sem):
    f = dwd.shape[0]
    copies = [
        pltpu.make_async_copy(dx, dx_hbm, sem.at[0]),
        pltpu.make_async_copy(dw.at[:, pl.ds(0, f)], dwg_hbm, sem.at[1]),
        pltpu.make_async_copy(dw.at[:, pl.ds(f, f)], dwu_hbm, sem.at[2]),
        pltpu.make_async_copy(dwd, dwd_hbm, sem.at[3]),
    ]
    for c in copies:
        c.start()
    for c in copies:
        c.wait()


def solution(mesh):
    assert mesh.shape["tp"] == 2 * CHIPS

    def step(x, dy, gate, up, w_gate, w_up, w_down):
        tokens, d = x.shape
        f = w_down.shape[0]
        assert tokens == CHIPS * 2 * BLOCK
        half = d // 2
        bf16, f32 = jnp.bfloat16, jnp.float32
        dma = pltpu.SemaphoreType.DMA
        vmem, hbm = pl.BlockSpec(memory_space=pltpu.VMEM), pl.BlockSpec(memory_space=pltpu.HBM)
        dx, dw, dwd = pl.pallas_call(
            main_kernel,
            name="block_grads",
            out_shape=(pltpu.VMEM((tokens, d), bf16), pltpu.VMEM((d, 2 * f), bf16), pltpu.VMEM((f, d), bf16)),
            in_specs=[hbm] * 7,
            out_specs=(vmem,) * 3,
            scratch_shapes=[
                pltpu.VMEM((tokens, d), bf16),
                pltpu.VMEM((tokens, d), bf16),
                pltpu.VMEM((tokens, 2 * f), bf16),
                pltpu.VMEM((d, 2 * f), bf16),
                pltpu.VMEM((f, d), bf16),
                pltpu.VMEM((BLOCK, f), bf16),
                pltpu.VMEM((f, tokens), bf16),
                pltpu.VMEM((BLOCK, f), f32),
                pltpu.VMEM((BLOCK, half), f32),
                pltpu.VMEM((2, BLOCK, half), bf16),
                pltpu.VMEM((6, 2, PART, half), bf16),
                pltpu.VMEM((2, 2, PART, half), bf16),
                pltpu.VMEM((2, 2, 2, PART, half), bf16),
                dma((3,)),
                dma((4, 8)),
                dma((2,)),
                dma((8,)),
                dma((6, 2)),
                dma((2, 2)),
                dma((2, 2, 2)),
                dma((2, 2, 2)),
                dma((2, 2, 2)),
                dma((2, 2)),
                dma((2, 2)),
                dma((14,)),
                dma((14,)),
            ],
            compiler_params=pltpu.CompilerParams(collective_id=0, has_side_effects=True, vmem_limit_bytes=44 * 2**20),
        )(x, dy, gate, up, w_gate, w_up, w_down)
        return pl.pallas_call(
            write_kernel,
            name="write_out",
            out_shape=tuple(
                jax.ShapeDtypeStruct(s, bf16) for s in ((tokens, d), (d, f), (d, f), (f, d))
            ),
            in_specs=[vmem] * 3,
            out_specs=(hbm,) * 4,
            scratch_shapes=[dma((4,))],
            compiler_params=pltpu.CompilerParams(vmem_limit_bytes=20 * 2**20),
        )(dx, dw, dwd)

    tokens, columns, rows = P("dp", None), P(None, "tp"), P("tp", None)
    return jax.shard_map(
        step,
        mesh=mesh,
        in_specs=(tokens, tokens, P("dp", "tp"), P("dp", "tp"), columns, columns, rows),
        out_specs=(tokens, P("dp", "tp"), P("dp", "tp"), P(("dp", "tp"), None)),
        check_vma=False,
    )
```

```python
import functools

import jax
import jax.numpy as jnp
from jax import lax
from jax.experimental import pallas as pl
from jax.experimental.pallas import tpu as pltpu
from jax.sharding import PartitionSpec as P

MESH = pl.DeviceIdType.MESH
CHIPS = 4
BLOCK = 256
PART = BLOCK // 2
PIECES = 2
SHARE = 32
STRIP = 32
TILE = 256


def act(gate, up):
    return jax.nn.gelu(gate) * up


def dot(a, b, contract):
    return lax.dot_general(a, b, ((contract[:1], contract[1:]), ((), ())), preferred_element_type=jnp.float32)


def main_kernel(
    x_hbm, dy_hbm, gate_hbm, up_hbm, wg_hbm, wu_hbm, wd_hbm,
    dx, dw, dwd,
    x, dy, gu, w, wd, hid, hid_t, dh, own, stage, sendbuf, far, near,
    in_sem, row_sem, term_send, term_recv, rs_send, far_recv, near_recv,
    ag_send, ag_recv, fwd_send, fwd_recv, peer_send, peer_recv,
):
    tokens, d = x.shape
    f = wd.shape[0]
    half = d // 2
    chunk_rows = tokens // CHIPS
    width = half // PIECES
    me = lax.axis_index("tp")
    chip, core = lax.div(me, 2), lax.rem(me, 2)
    peer = chip * 2 + 1 - core
    mine = pl.ds(pl.multiple_of(core * half, half), half)

    def chip_at(step):
        return lax.rem(chip + step, CHIPS)

    def device_at(step):
        return chip_at(step) * 2 + core

    steps = (1, CHIPS - 1)

    barrier = pltpu.get_barrier_semaphore()
    for other in (device_at(1), device_at(CHIPS - 1), peer):
        pl.semaphore_signal(barrier, inc=1, device_id={"tp": other}, device_id_type=MESH)

    def remote(src, dst, send, recv, device):
        return pltpu.make_async_remote_copy(
            src_ref=src, dst_ref=dst, send_sem=send, recv_sem=recv, device_id={"tp": device}, device_id_type=MESH
        )

    def row_at(step, i, p=0):
        return pl.multiple_of(chip_at(step) * chunk_rows + i * BLOCK + p * PART, PART)

    def row_copies(b, step, i):
        r = pl.ds(row_at(step, i), BLOCK)
        return (
            pltpu.make_async_copy(dy_hbm.at[r], dy.at[r], row_sem.at[0, b]),
            pltpu.make_async_copy(gate_hbm.at[r], gu.at[r, pl.ds(0, f)], row_sem.at[1, b]),
            pltpu.make_async_copy(up_hbm.at[r], gu.at[r, pl.ds(f, f)], row_sem.at[2, b]),
        )

    def start_rows(b, step, i):
        for c in row_copies(b, step, i):
            c.start()

    def x_copy(b):
        r = pl.ds(pl.multiple_of(b * BLOCK, BLOCK), BLOCK)
        return pltpu.make_async_copy(x_hbm.at[r], x.at[r], row_sem.at[3, b])

    in_wd = pltpu.make_async_copy(wd_hbm, wd, in_sem.at[0])
    in_wg = pltpu.make_async_copy(wg_hbm, w.at[:, pl.ds(0, f)], in_sem.at[1])
    in_wu = pltpu.make_async_copy(wu_hbm, w.at[:, pl.ds(f, f)], in_sem.at[2])
    in_wd.start()
    start_rows(0, 2, 0)
    in_wg.start()
    in_wu.start()
    start_rows(1, 2, 1)

    def hidden_block(b, step, i):
        start = row_at(step, i)
        for c in row_copies(b, step, i):
            c.wait()
        dh[...] = dot(dy[pl.ds(start, BLOCK), :], wd[...], (1, 1))

        @pl.loop(0, BLOCK // STRIP)
        def _(s):
            here = pl.ds(pl.multiple_of(s * STRIP, STRIP), STRIP)
            r = pl.ds(pl.multiple_of(start + s * STRIP, STRIP), STRIP)
            h, back = jax.vjp(act, gu[r, pl.ds(0, f)].astype(jnp.float32), gu[r, pl.ds(f, f)].astype(jnp.float32))
            d_gate, d_up = back(dh[here, :])
            gu[r, pl.ds(0, f)] = d_gate.astype(gu.dtype)
            gu[r, pl.ds(f, f)] = d_up.astype(gu.dtype)
            hid[here, :] = h.astype(hid.dtype)

        hid_t[:, pl.ds(pl.multiple_of(start, BLOCK), BLOCK)] = hid[...].T

    def cols_of(c, q):
        return pl.ds(pl.multiple_of(c * half + q * width, width), width)

    def term_copy(b, step, i, slot, q):
        rows = pl.ds(row_at(step, i), BLOCK)
        return remote(
            stage.at[slot, q], dx.at[rows, cols_of(1 - core, q)], term_send.at[slot, q], term_recv.at[b, q], peer
        )

    def term_other(b, step, i, slot):
        rows = pl.ds(row_at(step, i), BLOCK)
        for q in range(PIECES):
            stage[slot, q] = dot(gu[rows, :], w[cols_of(1 - core, q), :], (1, 1)).astype(stage.dtype)
            term_copy(b, step, i, slot, q).start()

    def term_own(step, i, slot):
        rows = pl.ds(row_at(step, i), BLOCK)
        for q in range(PIECES):
            own[slot, q] = dot(gu[rows, :], w[cols_of(core, q), :], (1, 1))

    def stage_free(slot):
        for q in range(PIECES):
            term_copy(0, 0, 0, slot, q).wait_send()

    def summed(step, i, p, q, slot):
        r = pl.ds(row_at(step, i, p), PART)
        mine_here = own[slot, q, pl.ds(pl.multiple_of(p * PART, PART), PART), :]
        return mine_here + dx[r, cols_of(core, q)].astype(jnp.float32)

    def far_copy(i, side, q):
        return remote(
            sendbuf.at[i, side, q],
            far.at[side, i, q],
            rs_send.at[i, side, q],
            far_recv.at[side, i, q],
            device_at(steps[side]),
        )

    def near_copy(j, i, p, q, side, step):
        return remote(
            sendbuf.at[2 + j, p, q],
            near.at[side, i, p, q],
            rs_send.at[2 + j, p, q],
            near_recv.at[side, i, p, q],
            device_at(step),
        )

    def finish_far(i):
        for q in range(PIECES):
            term_copy(i, 2, i, i, q).wait_recv()
            for p in range(2):
                sendbuf[i, p, q] = summed(2, i, p, q, i).astype(sendbuf.dtype)
                far_copy(i, p, q).start()

    in_wd.wait()

    hidden_block(0, 2, 0)
    start_rows(2, 1, 0)
    x_copy(0).start()
    in_wg.wait()
    in_wu.wait()
    pl.semaphore_wait(barrier, 3)
    term_other(0, 2, 0, 0)
    term_own(2, 0, 0)
    finish_far(0)

    hidden_block(1, 2, 1)
    start_rows(3, 3, 0)
    x_copy(1).start()
    term_other(1, 2, 1, 1)
    hidden_block(2, 1, 0)
    term_own(2, 1, 1)
    finish_far(1)

    @pl.loop(0, 4)
    def _(j):
        side, i = lax.rem(j, 2), lax.div(j, 2)
        step = 1 + 2 * side

        @pl.when(j < 2)
        def _():
            start_rows(4 + j, step, 1)

        @pl.when(j >= 2)
        def _():
            start_rows(4 + j, 0, side)

        x_copy(2 + j).start()
        stage_free(side)
        term_other(2 + j, step, i, side)
        more = 1 - lax.div(j, 3)
        hidden_block(3 + j, (3 - 2 * side) * more, lax.div(j + 1, 2) * more)
        term_own(step, i, side)
        plain = 1 - side
        for q in range(PIECES):
            term_copy(2 + j, step, i, side, q).wait_recv()
            sendbuf[2 + j, plain, q] = summed(step, i, plain, q, side).astype(sendbuf.dtype)
            near_copy(j, i, plain, q, side, step).start()
        for q in range(PIECES):
            remote(sendbuf.at[0, 0, 0], far.at[side, i, q], rs_send.at[0, 0, 0], far_recv.at[side, i, q], peer).wait_recv()
            sendbuf[2 + j, side, q] = (
                summed(step, i, side, q, side) + far[side, i, q].astype(jnp.float32)
            ).astype(sendbuf.dtype)
            near_copy(j, i, side, q, side, step).start()

    x_copy(6).start()
    x_copy(7).start()
    stage_free(0)
    term_other(6, 0, 0, 0)
    hidden_block(7, 0, 1)
    term_own(0, 0, 0)
    stage_free(1)
    term_other(7, 0, 1, 1)
    term_own(0, 1, 1)

    @pl.loop(0, 4)
    def _(t):
        cols = pl.ds(pl.multiple_of(t * (d // 4), d // 4), d // 4)
        dwd[:, cols] = dot(hid_t[...], dy[:, cols], (1, 0)).astype(dwd.dtype)

    def direct(i, p, side):
        r = pl.ds(row_at(0, i, p), PART)
        return remote(
            dx.at[r, mine], dx.at[r, mine], ag_send.at[side, i, p], ag_recv.at[side, i, p], device_at(steps[side])
        )

    def forward(i, side, k):
        r = pl.ds(pl.multiple_of(row_at(steps[1 - side], i, side) + k * SHARE, SHARE), SHARE)
        return remote(
            dx.at[r, mine], dx.at[r, mine], fwd_send.at[side, i, k], fwd_recv.at[side, i, k], device_at(steps[side])
        )

    peers = []

    def share(step, i, p, rows=PART, k=0):
        n, r = len(peers), pl.ds(pl.multiple_of(row_at(step, i, p) + k * SHARE, SHARE), rows)
        peers.append(remote(dx.at[r, mine], dx.at[r, mine], peer_send.at[n], peer_recv.at[n], peer))
        peers[-1].start()

    def own_block(i):
        for q in range(PIECES):
            term_copy(6 + i, 0, i, i, q).wait_recv()
        for p in range(2):
            for q in range(PIECES):
                total = summed(0, i, p, q, i)
                for side in range(2):
                    near_copy(0, i, p, q, side, 0).wait_recv()
                    total += near[side, i, p, q].astype(jnp.float32)
                dx[pl.ds(row_at(0, i, p), PART), cols_of(core, q)] = total.astype(dx.dtype)
            direct(i, p, p).start()
        direct(i, 1, 0).start()
        direct(i, 0, 1).start()
        share(0, i, 0, BLOCK)

    def weight_tiles(lo, hi):
        @pl.loop(lo, hi)
        def _(t):
            cols = pl.ds(pl.multiple_of(t * TILE, TILE), TILE)
            dw[cols, :] = dot(x[:, cols], gu[...], (0, 0)).astype(dw.dtype)

    def relay(i):
        for side in range(2):
            direct(i, side, side).wait_recv()
            for k in range(PART // SHARE):
                forward(i, side, k).start()
            share(steps[1 - side], i, side)

    def keep(i):
        for side in range(2):
            direct(i, 1 - side, side).wait_recv()
            share(steps[1 - side], i, 1 - side)

    def last(i):
        for k in range(PART // SHARE):
            for side in range(2):
                forward(i, side, k).wait_recv()
                share(2, i, side, SHARE, k)

    own_block(0)
    for b in range(8):
        x_copy(b).wait()
    weight_tiles(0, 5)
    own_block(1)
    weight_tiles(5, d // TILE)
    relay(0)
    keep(0)
    relay(1)
    keep(1)
    last(0)
    last(1)

    for i in range(2):
        stage_free(i)
        for p in range(2):
            for q in range(PIECES):
                far_copy(i, p, q).wait_send()
                for side in range(2):
                    near_copy(2 * i + side, i, p, q, side, steps[side]).wait_send()
            for side in range(2):
                direct(i, p, side).wait_send()
        for side in range(2):
            for k in range(PART // SHARE):
                forward(i, side, k).wait_send()
    for c in peers:
        c.wait()


def write_kernel(dx, dw, dwd, dx_hbm, dwg_hbm, dwu_hbm, dwd_hbm, sem):
    f = dwd.shape[0]
    copies = [
        pltpu.make_async_copy(dx, dx_hbm, sem.at[0]),
        pltpu.make_async_copy(dw.at[:, pl.ds(0, f)], dwg_hbm, sem.at[1]),
        pltpu.make_async_copy(dw.at[:, pl.ds(f, f)], dwu_hbm, sem.at[2]),
        pltpu.make_async_copy(dwd, dwd_hbm, sem.at[3]),
    ]
    for c in copies:
        c.start()
    for c in copies:
        c.wait()


def solution(mesh):
    assert mesh.shape["tp"] == 2 * CHIPS

    def step(x, dy, gate, up, w_gate, w_up, w_down):
        tokens, d = x.shape
        f = w_down.shape[0]
        assert tokens == CHIPS * 2 * BLOCK
        half = d // 2
        bf16, f32 = jnp.bfloat16, jnp.float32
        dma = pltpu.SemaphoreType.DMA
        vmem, hbm = pl.BlockSpec(memory_space=pltpu.VMEM), pl.BlockSpec(memory_space=pltpu.HBM)
        dx, dw, dwd = pl.pallas_call(
            main_kernel,
            name="block_grads",
            out_shape=(pltpu.VMEM((tokens, d), bf16), pltpu.VMEM((d, 2 * f), bf16), pltpu.VMEM((f, d), bf16)),
            in_specs=[hbm] * 7,
            out_specs=(vmem,) * 3,
            scratch_shapes=[
                pltpu.VMEM((tokens, d), bf16),
                pltpu.VMEM((tokens, d), bf16),
                pltpu.VMEM((tokens, 2 * f), bf16),
                pltpu.VMEM((d, 2 * f), bf16),
                pltpu.VMEM((f, d), bf16),
                pltpu.VMEM((BLOCK, f), bf16),
                pltpu.VMEM((f, tokens), bf16),
                pltpu.VMEM((BLOCK, f), f32),
                pltpu.VMEM((2, PIECES, BLOCK, half // PIECES), f32),
                pltpu.VMEM((2, PIECES, BLOCK, half // PIECES), bf16),
                pltpu.VMEM((6, 2, PIECES, PART, half // PIECES), bf16),
                pltpu.VMEM((2, 2, PIECES, PART, half // PIECES), bf16),
                pltpu.VMEM((2, 2, 2, PIECES, PART, half // PIECES), bf16),
                dma((3,)),
                dma((4, 8)),
                dma((2, PIECES)),
                dma((8, PIECES)),
                dma((6, 2, PIECES)),
                dma((2, 2, PIECES)),
                dma((2, 2, 2, PIECES)),
                dma((2, 2, 2)),
                dma((2, 2, 2)),
                dma((2, 2, PART // SHARE)),
                dma((2, 2, PART // SHARE)),
                dma((10 + 4 * PART // SHARE,)),
                dma((10 + 4 * PART // SHARE,)),
            ],
            compiler_params=pltpu.CompilerParams(collective_id=0, has_side_effects=True, vmem_limit_bytes=47 * 2**20),
        )(x, dy, gate, up, w_gate, w_up, w_down)
        return pl.pallas_call(
            write_kernel,
            name="write_out",
            out_shape=tuple(
                jax.ShapeDtypeStruct(s, bf16) for s in ((tokens, d), (d, f), (d, f), (f, d))
            ),
            in_specs=[vmem] * 3,
            out_specs=(hbm,) * 4,
            scratch_shapes=[dma((4,))],
            compiler_params=pltpu.CompilerParams(vmem_limit_bytes=20 * 2**20),
        )(dx, dw, dwd)

    tokens, columns, rows = P("dp", None), P(None, "tp"), P("tp", None)
    return jax.shard_map(
        step,
        mesh=mesh,
        in_specs=(tokens, tokens, P("dp", "tp"), P("dp", "tp"), columns, columns, rows),
        out_specs=(tokens, P("dp", "tp"), P("dp", "tp"), P(("dp", "tp"), None)),
        check_vma=False,
    )
```

```python
import functools

import jax
import jax.numpy as jnp
from jax import lax
from jax.experimental import pallas as pl
from jax.experimental.pallas import tpu as pltpu
from jax.sharding import PartitionSpec as P

MESH = pl.DeviceIdType.MESH
CHIPS = 4
BLOCK = 256
PART = BLOCK // 2
PIECES = 2
SHARE = 32
STRIP = 32
TILE = 256


def act(gate, up):
    return jax.nn.gelu(gate) * up


def dot(a, b, contract):
    return lax.dot_general(a, b, ((contract[:1], contract[1:]), ((), ())), preferred_element_type=jnp.float32)


def main_kernel(
    x_hbm, dy_hbm, gate_hbm, up_hbm, wg_hbm, wu_hbm, wd_hbm,
    dx, dw, dwd,
    x, dy, gu, w, wd, hid, hid_t, dh, own, stage, sendbuf, far, near,
    in_sem, row_sem, term_send, term_recv, rs_send, far_recv, near_recv,
    ag_send, ag_recv, fwd_send, fwd_recv, peer_send, peer_recv,
):
    tokens, d = x.shape
    f = wd.shape[0]
    half = d // 2
    chunk_rows = tokens // CHIPS
    width = half // PIECES
    me = lax.axis_index("tp")
    chip, core = lax.div(me, 2), lax.rem(me, 2)
    peer = chip * 2 + 1 - core
    mine = pl.ds(pl.multiple_of(core * half, half), half)

    def chip_at(step):
        return lax.rem(chip + step, CHIPS)

    def device_at(step):
        return chip_at(step) * 2 + core

    steps = (1, CHIPS - 1)

    barrier = pltpu.get_barrier_semaphore()
    for other in (device_at(1), device_at(CHIPS - 1), peer):
        pl.semaphore_signal(barrier, inc=1, device_id={"tp": other}, device_id_type=MESH)

    def remote(src, dst, send, recv, device):
        return pltpu.make_async_remote_copy(
            src_ref=src, dst_ref=dst, send_sem=send, recv_sem=recv, device_id={"tp": device}, device_id_type=MESH
        )

    def row_at(step, i, p=0):
        return pl.multiple_of(chip_at(step) * chunk_rows + i * BLOCK + p * PART, PART)

    def row_copies(b, step, i):
        r = pl.ds(row_at(step, i), BLOCK)
        return (
            pltpu.make_async_copy(dy_hbm.at[r], dy.at[r], row_sem.at[0, b]),
            pltpu.make_async_copy(gate_hbm.at[r], gu.at[r, pl.ds(0, f)], row_sem.at[1, b]),
            pltpu.make_async_copy(up_hbm.at[r], gu.at[r, pl.ds(f, f)], row_sem.at[2, b]),
        )

    def start_rows(b, step, i):
        for c in row_copies(b, step, i):
            c.start()

    def x_copy(b):
        r = pl.ds(pl.multiple_of(b * BLOCK, BLOCK), BLOCK)
        return pltpu.make_async_copy(x_hbm.at[r], x.at[r], row_sem.at[3, b])

    in_wd = pltpu.make_async_copy(wd_hbm, wd, in_sem.at[0])
    in_wg = pltpu.make_async_copy(wg_hbm, w.at[:, pl.ds(0, f)], in_sem.at[1])
    in_wu = pltpu.make_async_copy(wu_hbm, w.at[:, pl.ds(f, f)], in_sem.at[2])
    in_wd.start()
    start_rows(0, 2, 0)
    in_wg.start()
    in_wu.start()
    start_rows(1, 2, 1)

    def hidden_block(b, step, i):
        start = row_at(step, i)
        for c in row_copies(b, step, i):
            c.wait()
        dh[...] = dot(dy[pl.ds(start, BLOCK), :], wd[...], (1, 1))

        @pl.loop(0, BLOCK // STRIP)
        def _(s):
            here = pl.ds(pl.multiple_of(s * STRIP, STRIP), STRIP)
            r = pl.ds(pl.multiple_of(start + s * STRIP, STRIP), STRIP)
            h, back = jax.vjp(act, gu[r, pl.ds(0, f)].astype(jnp.float32), gu[r, pl.ds(f, f)].astype(jnp.float32))
            d_gate, d_up = back(dh[here, :])
            gu[r, pl.ds(0, f)] = d_gate.astype(gu.dtype)
            gu[r, pl.ds(f, f)] = d_up.astype(gu.dtype)
            hid[here, :] = h.astype(hid.dtype)

        hid_t[:, pl.ds(pl.multiple_of(start, BLOCK), BLOCK)] = hid[...].T

    def cols_of(c, q):
        return pl.ds(pl.multiple_of(c * half + q * width, width), width)

    def term_copy(b, step, i, slot, q):
        rows = pl.ds(row_at(step, i), BLOCK)
        return remote(
            stage.at[slot, q], dx.at[rows, cols_of(1 - core, q)], term_send.at[slot, q], term_recv.at[b, q], peer
        )

    def term_other(b, step, i, slot):
        rows = pl.ds(row_at(step, i), BLOCK)
        for q in range(PIECES):
            stage[slot, q] = dot(gu[rows, :], w[cols_of(1 - core, q), :], (1, 1)).astype(stage.dtype)
            term_copy(b, step, i, slot, q).start()

    def term_own(step, i, slot):
        rows = pl.ds(row_at(step, i), BLOCK)
        for q in range(PIECES):
            own[slot, q] = dot(gu[rows, :], w[cols_of(core, q), :], (1, 1))

    def stage_free(slot):
        for q in range(PIECES):
            term_copy(0, 0, 0, slot, q).wait_send()

    def summed(step, i, p, q, slot):
        r = pl.ds(row_at(step, i, p), PART)
        mine_here = own[slot, q, pl.ds(pl.multiple_of(p * PART, PART), PART), :]
        return mine_here + dx[r, cols_of(core, q)].astype(jnp.float32)

    def far_copy(i, side, q):
        return remote(
            sendbuf.at[i, side, q],
            far.at[side, i, q],
            rs_send.at[i, side, q],
            far_recv.at[side, i, q],
            device_at(steps[side]),
        )

    def near_copy(j, i, p, q, side, step):
        return remote(
            sendbuf.at[2 + j, p, q],
            near.at[side, i, p, q],
            rs_send.at[2 + j, p, q],
            near_recv.at[side, i, p, q],
            device_at(step),
        )

    def finish_far(i):
        for q in range(PIECES):
            term_copy(i, 2, i, i, q).wait_recv()
            for p in range(2):
                sendbuf[i, p, q] = summed(2, i, p, q, i).astype(sendbuf.dtype)
                far_copy(i, p, q).start()

    in_wd.wait()

    hidden_block(0, 2, 0)
    start_rows(2, 1, 0)
    x_copy(0).start()
    in_wg.wait()
    in_wu.wait()
    pl.semaphore_wait(barrier, 3)
    term_other(0, 2, 0, 0)
    term_own(2, 0, 0)
    finish_far(0)

    hidden_block(1, 2, 1)
    start_rows(3, 3, 0)
    x_copy(1).start()
    term_other(1, 2, 1, 1)
    hidden_block(2, 1, 0)
    term_own(2, 1, 1)
    finish_far(1)

    @pl.loop(0, 2)
    def _(i):
        for side in range(2):
            b, step, plain = 2 + 2 * i + side, steps[side], 1 - side

            @pl.when(i == 0)
            def _():
                start_rows(4 + side, step, 1)

            @pl.when(i == 1)
            def _():
                start_rows(6 + side, 0, side)

            x_copy(b).start()
            stage_free(side)
            term_other(b, step, i, side)
            if side == 0:
                hidden_block(b + 1, steps[1], i)
            else:
                hidden_block(b + 1, 1 - i, 1 - i)
            term_own(step, i, side)
            for q in range(PIECES):
                term_copy(b, step, i, side, q).wait_recv()
                sendbuf[b, plain, q] = summed(step, i, plain, q, side).astype(sendbuf.dtype)
                near_copy(b - 2, i, plain, q, side, step).start()
        for q in range(PIECES):
            for side in range(2):
                b, step = 2 + 2 * i + side, steps[side]
                far_copy(i, side, q).wait_recv()
                sendbuf[b, side, q] = (
                    summed(step, i, side, q, side) + far[side, i, q].astype(jnp.float32)
                ).astype(sendbuf.dtype)
                near_copy(b - 2, i, side, q, side, step).start()

    x_copy(6).start()
    x_copy(7).start()
    stage_free(0)
    term_other(6, 0, 0, 0)
    hidden_block(7, 0, 1)
    term_own(0, 0, 0)
    stage_free(1)
    term_other(7, 0, 1, 1)
    term_own(0, 1, 1)

    @pl.loop(0, 4)
    def _(t):
        cols = pl.ds(pl.multiple_of(t * (d // 4), d // 4), d // 4)
        dwd[:, cols] = dot(hid_t[...], dy[:, cols], (1, 0)).astype(dwd.dtype)

    def direct(i, p, side):
        r = pl.ds(row_at(0, i, p), PART)
        return remote(
            dx.at[r, mine], dx.at[r, mine], ag_send.at[side, i, p], ag_recv.at[side, i, p], device_at(steps[side])
        )

    def forward(i, side, k):
        r = pl.ds(pl.multiple_of(row_at(steps[1 - side], i, side) + k * SHARE, SHARE), SHARE)
        return remote(
            dx.at[r, mine], dx.at[r, mine], fwd_send.at[side, i, k], fwd_recv.at[side, i, k], device_at(steps[side])
        )

    peers = []

    def share(step, i, p, rows=PART, k=0):
        n, r = len(peers), pl.ds(pl.multiple_of(row_at(step, i, p) + k * SHARE, SHARE), rows)
        peers.append(remote(dx.at[r, mine], dx.at[r, mine], peer_send.at[n], peer_recv.at[n], peer))
        peers[-1].start()

    def own_block(i):
        for q in range(PIECES):
            term_copy(6 + i, 0, i, i, q).wait_recv()
        for p in range(2):
            for q in range(PIECES):
                total = summed(0, i, p, q, i)
                for side in range(2):
                    near_copy(0, i, p, q, side, 0).wait_recv()
                    total += near[side, i, p, q].astype(jnp.float32)
                dx[pl.ds(row_at(0, i, p), PART), cols_of(core, q)] = total.astype(dx.dtype)
            direct(i, p, p).start()
        direct(i, 1, 0).start()
        direct(i, 0, 1).start()
        share(0, i, 0, BLOCK)

    def weight_tiles(lo, hi):
        @pl.loop(lo, hi)
        def _(t):
            cols = pl.ds(pl.multiple_of(t * TILE, TILE), TILE)
            dw[cols, :] = dot(x[:, cols], gu[...], (0, 0)).astype(dw.dtype)

    def relay(i):
        for side in range(2):
            direct(i, side, side).wait_recv()
            for k in range(PART // SHARE):
                forward(i, side, k).start()
            share(steps[1 - side], i, side)

    def keep(i):
        for side in range(2):
            direct(i, 1 - side, side).wait_recv()
            share(steps[1 - side], i, 1 - side)

    def last(i):
        for k in range(PART // SHARE):
            for side in range(2):
                forward(i, side, k).wait_recv()
                share(2, i, side, SHARE, k)

    own_block(0)
    for b in range(8):
        x_copy(b).wait()
    weight_tiles(0, 5)
    own_block(1)
    weight_tiles(5, d // TILE)
    relay(0)
    keep(0)
    relay(1)
    keep(1)
    last(0)
    last(1)

    for i in range(2):
        stage_free(i)
        for p in range(2):
            for q in range(PIECES):
                far_copy(i, p, q).wait_send()
                for side in range(2):
                    near_copy(2 * i + side, i, p, q, side, steps[side]).wait_send()
            for side in range(2):
                direct(i, p, side).wait_send()
        for side in range(2):
            for k in range(PART // SHARE):
                forward(i, side, k).wait_send()
    for c in peers:
        c.wait()


def write_kernel(dx, dw, dwd, dx_hbm, dwg_hbm, dwu_hbm, dwd_hbm, sem):
    f = dwd.shape[0]
    copies = [
        pltpu.make_async_copy(dx, dx_hbm, sem.at[0]),
        pltpu.make_async_copy(dw.at[:, pl.ds(0, f)], dwg_hbm, sem.at[1]),
        pltpu.make_async_copy(dw.at[:, pl.ds(f, f)], dwu_hbm, sem.at[2]),
        pltpu.make_async_copy(dwd, dwd_hbm, sem.at[3]),
    ]
    for c in copies:
        c.start()
    for c in copies:
        c.wait()


def solution(mesh):
    assert mesh.shape["tp"] == 2 * CHIPS

    def step(x, dy, gate, up, w_gate, w_up, w_down):
        tokens, d = x.shape
        f = w_down.shape[0]
        assert tokens == CHIPS * 2 * BLOCK
        half = d // 2
        bf16, f32 = jnp.bfloat16, jnp.float32
        dma = pltpu.SemaphoreType.DMA
        vmem, hbm = pl.BlockSpec(memory_space=pltpu.VMEM), pl.BlockSpec(memory_space=pltpu.HBM)
        dx, dw, dwd = pl.pallas_call(
            main_kernel,
            name="block_grads",
            out_shape=(pltpu.VMEM((tokens, d), bf16), pltpu.VMEM((d, 2 * f), bf16), pltpu.VMEM((f, d), bf16)),
            in_specs=[hbm] * 7,
            out_specs=(vmem,) * 3,
            scratch_shapes=[
                pltpu.VMEM((tokens, d), bf16),
                pltpu.VMEM((tokens, d), bf16),
                pltpu.VMEM((tokens, 2 * f), bf16),
                pltpu.VMEM((d, 2 * f), bf16),
                pltpu.VMEM((f, d), bf16),
                pltpu.VMEM((BLOCK, f), bf16),
                pltpu.VMEM((f, tokens), bf16),
                pltpu.VMEM((BLOCK, f), f32),
                pltpu.VMEM((2, PIECES, BLOCK, half // PIECES), f32),
                pltpu.VMEM((2, PIECES, BLOCK, half // PIECES), bf16),
                pltpu.VMEM((6, 2, PIECES, PART, half // PIECES), bf16),
                pltpu.VMEM((2, 2, PIECES, PART, half // PIECES), bf16),
                pltpu.VMEM((2, 2, 2, PIECES, PART, half // PIECES), bf16),
                dma((3,)),
                dma((4, 8)),
                dma((2, PIECES)),
                dma((8, PIECES)),
                dma((6, 2, PIECES)),
                dma((2, 2, PIECES)),
                dma((2, 2, 2, PIECES)),
                dma((2, 2, 2)),
                dma((2, 2, 2)),
                dma((2, 2, PART // SHARE)),
                dma((2, 2, PART // SHARE)),
                dma((10 + 4 * PART // SHARE,)),
                dma((10 + 4 * PART // SHARE,)),
            ],
            compiler_params=pltpu.CompilerParams(collective_id=0, has_side_effects=True, vmem_limit_bytes=47 * 2**20),
        )(x, dy, gate, up, w_gate, w_up, w_down)
        return pl.pallas_call(
            write_kernel,
            name="write_out",
            out_shape=tuple(
                jax.ShapeDtypeStruct(s, bf16) for s in ((tokens, d), (d, f), (d, f), (f, d))
            ),
            in_specs=[vmem] * 3,
            out_specs=(hbm,) * 4,
            scratch_shapes=[dma((4,))],
            compiler_params=pltpu.CompilerParams(vmem_limit_bytes=20 * 2**20),
        )(dx, dw, dwd)

    tokens, columns, rows = P("dp", None), P(None, "tp"), P("tp", None)
    return jax.shard_map(
        step,
        mesh=mesh,
        in_specs=(tokens, tokens, P("dp", "tp"), P("dp", "tp"), columns, columns, rows),
        out_specs=(tokens, P("dp", "tp"), P("dp", "tp"), P(("dp", "tp"), None)),
        check_vma=False,
    )
```

```python
import functools

import jax
import jax.numpy as jnp
from jax import lax
from jax.experimental import pallas as pl
from jax.experimental.pallas import tpu as pltpu
from jax.sharding import PartitionSpec as P

MESH = pl.DeviceIdType.MESH
CHIPS = 4
BLOCK = 256
PART = BLOCK // 2
PIECES = 2
SHARE = 32
STRIP = 32
TILE = 256


def act(gate, up):
    return jax.nn.gelu(gate) * up


def dot(a, b, contract):
    return lax.dot_general(a, b, ((contract[:1], contract[1:]), ((), ())), preferred_element_type=jnp.float32)


def main_kernel(
    x_hbm, dy_hbm, gate_hbm, up_hbm, wg_hbm, wu_hbm, wd_hbm,
    dx, dw, dwd,
    x, dy, gu, w, wd, hid, hid_t, dh, own, stage, sendbuf, far, near,
    in_sem, row_sem, x_sem, term_send, term_recv, rs_send, far_recv, near_recv,
    ag_send, ag_recv, fwd_send, fwd_recv, peer_send, peer_recv,
):
    tokens, d = x.shape
    f = wd.shape[0]
    half = d // 2
    chunk_rows = tokens // CHIPS
    width = half // PIECES
    me = lax.axis_index("tp")
    chip, core = lax.div(me, 2), lax.rem(me, 2)
    peer = chip * 2 + 1 - core
    mine = pl.ds(pl.multiple_of(core * half, half), half)

    def chip_at(step):
        return lax.rem(chip + step, CHIPS)

    def device_at(step):
        return chip_at(step) * 2 + core

    steps = (1, CHIPS - 1)

    barrier = pltpu.get_barrier_semaphore()
    for other in (device_at(1), device_at(CHIPS - 1), peer):
        pl.semaphore_signal(barrier, inc=1, device_id={"tp": other}, device_id_type=MESH)

    def remote(src, dst, send, recv, device):
        return pltpu.make_async_remote_copy(
            src_ref=src, dst_ref=dst, send_sem=send, recv_sem=recv, device_id={"tp": device}, device_id_type=MESH
        )

    def row_at(step, i, p=0):
        return pl.multiple_of(chip_at(step) * chunk_rows + i * BLOCK + p * PART, PART)

    def far_rows(i):
        return row_at(2, i, 0), row_at(2, i, 1)

    def near_rows(i, k):
        return row_at(1, i, 1 - k), row_at(CHIPS - 1, i, k)

    def own_rows(i):
        return row_at(0, i, 0), row_at(0, i, 1)

    def row_copies(b, rows):
        copies = []
        for p in range(2):
            r = pl.ds(rows[p], PART)
            copies += [
                pltpu.make_async_copy(dy_hbm.at[r], dy.at[r], row_sem.at[0, b, p]),
                pltpu.make_async_copy(gate_hbm.at[r], gu.at[r, pl.ds(0, f)], row_sem.at[1, b, p]),
                pltpu.make_async_copy(up_hbm.at[r], gu.at[r, pl.ds(f, f)], row_sem.at[2, b, p]),
            ]
        return copies

    def start_rows(b, rows):
        for c in row_copies(b, rows):
            c.start()

    def x_copy(b):
        r = pl.ds(pl.multiple_of(b * BLOCK, BLOCK), BLOCK)
        return pltpu.make_async_copy(x_hbm.at[r], x.at[r], x_sem.at[b])

    in_wd = pltpu.make_async_copy(wd_hbm, wd, in_sem.at[0])
    in_wg = pltpu.make_async_copy(wg_hbm, w.at[:, pl.ds(0, f)], in_sem.at[1])
    in_wu = pltpu.make_async_copy(wu_hbm, w.at[:, pl.ds(f, f)], in_sem.at[2])
    in_wd.start()
    start_rows(0, far_rows(0))
    in_wg.start()
    in_wu.start()
    start_rows(1, far_rows(1))

    def both(ref, rows):
        return jnp.concatenate([ref[pl.ds(r, PART), :] for r in rows], axis=0)

    def hidden_block(b, rows):
        for c in row_copies(b, rows):
            c.wait()
        dh[...] = dot(both(dy, rows), wd[...], (1, 1))
        for p in range(2):

            @pl.loop(0, PART // STRIP)
            def _(s):
                here = pl.ds(pl.multiple_of(p * PART + s * STRIP, STRIP), STRIP)
                r = pl.ds(pl.multiple_of(rows[p] + s * STRIP, STRIP), STRIP)
                h, back = jax.vjp(act, gu[r, pl.ds(0, f)].astype(jnp.float32), gu[r, pl.ds(f, f)].astype(jnp.float32))
                d_gate, d_up = back(dh[here, :])
                gu[r, pl.ds(0, f)] = d_gate.astype(gu.dtype)
                gu[r, pl.ds(f, f)] = d_up.astype(gu.dtype)
                hid[here, :] = h.astype(hid.dtype)

            hid_t[:, pl.ds(rows[p], PART)] = hid[p * PART : (p + 1) * PART, :].T

    def cols_of(c, q):
        return pl.ds(pl.multiple_of(c * half + q * width, width), width)

    def term_copy(b, rows, slot, q, p):
        return remote(
            stage.at[slot, q, pl.ds(p * PART, PART)],
            dx.at[pl.ds(rows[p], PART), cols_of(1 - core, q)],
            term_send.at[slot, q, p],
            term_recv.at[b, q, p],
            peer,
        )

    def term_other(b, rows, slot):
        for q in range(PIECES):
            stage[slot, q] = dot(both(gu, rows), w[cols_of(1 - core, q), :], (1, 1)).astype(stage.dtype)
            for p in range(2):
                term_copy(b, rows, slot, q, p).start()

    def term_own(rows, slot):
        for q in range(PIECES):
            own[slot, q] = dot(both(gu, rows), w[cols_of(core, q), :], (1, 1))

    def stage_free(slot):
        for q in range(PIECES):
            for p in range(2):
                term_copy(0, far_rows(0), slot, q, p).wait_send()

    def summed(b, rows, slot, q, p):
        term_copy(b, rows, slot, q, p).wait_recv()
        return own[slot, q, p * PART : (p + 1) * PART, :] + dx[pl.ds(rows[p], PART), cols_of(core, q)].astype(jnp.float32)

    def far_copy(i, side, q):
        return remote(
            sendbuf.at[i, side, q],
            far.at[side, i, q],
            rs_send.at[i, side, q],
            far_recv.at[side, i, q],
            device_at(steps[side]),
        )

    def near_copy(i, k, side, q):
        b = 2 + 2 * i + k
        return remote(
            sendbuf.at[b, side, q],
            near.at[side, i, k, q],
            rs_send.at[b, side, q],
            near_recv.at[side, i, k, q],
            device_at(steps[side]),
        )

    def finish_far(i):
        for q in range(PIECES):
            for side in range(2):
                sendbuf[i, side, q] = summed(i, far_rows(i), i, q, side).astype(sendbuf.dtype)
                far_copy(i, side, q).start()

    in_wd.wait()

    hidden_block(0, far_rows(0))
    start_rows(2, near_rows(0, 0))
    x_copy(0).start()
    in_wg.wait()
    in_wu.wait()
    pl.semaphore_wait(barrier, 3)
    term_other(0, far_rows(0), 0)
    term_own(far_rows(0), 0)
    finish_far(0)

    hidden_block(1, far_rows(1))
    start_rows(3, near_rows(0, 1))
    x_copy(1).start()
    term_other(1, far_rows(1), 1)
    hidden_block(2, near_rows(0, 0))
    term_own(far_rows(1), 1)
    finish_far(1)

    @pl.loop(0, 2)
    def _(i):
        m = 1 - i
        coming = (
            (row_at(m, m, m), row_at(3 * m, m, 1 - m)),
            (row_at(m, 1, 0), row_at(3 * m, 1, 1)),
        )
        for k in range(2):
            b, rows = 2 + 2 * i + k, near_rows(i, k)
            start_rows(b + 2, coming[k])
            x_copy(b).start()
            stage_free(k)
            term_other(b, rows, k)
            hidden_block(b + 1, near_rows(i, 1) if k == 0 else coming[0])
            term_own(rows, k)
            for q in range(PIECES):
                for side in range(2):
                    total = summed(b, rows, k, q, side)
                    if k == 1:
                        far_copy(i, side, q).wait_recv()
                        total += far[side, i, q].astype(jnp.float32)
                    sendbuf[b, side, q] = total.astype(sendbuf.dtype)
                    near_copy(i, k, side, q).start()

    x_copy(6).start()
    x_copy(7).start()
    stage_free(0)
    term_other(6, own_rows(0), 0)
    hidden_block(7, own_rows(1))
    term_own(own_rows(0), 0)
    stage_free(1)
    term_other(7, own_rows(1), 1)
    term_own(own_rows(1), 1)

    @pl.loop(0, 4)
    def _(t):
        cols = pl.ds(pl.multiple_of(t * (d // 4), d // 4), d // 4)
        dwd[:, cols] = dot(hid_t[...], dy[:, cols], (1, 0)).astype(dwd.dtype)

    def direct(i, p, side):
        r = pl.ds(row_at(0, i, p), PART)
        return remote(
            dx.at[r, mine], dx.at[r, mine], ag_send.at[side, i, p], ag_recv.at[side, i, p], device_at(steps[side])
        )

    def forward(i, side, k):
        r = pl.ds(pl.multiple_of(row_at(steps[1 - side], i, side) + k * SHARE, SHARE), SHARE)
        return remote(
            dx.at[r, mine], dx.at[r, mine], fwd_send.at[side, i, k], fwd_recv.at[side, i, k], device_at(steps[side])
        )

    peers = []

    def share(step, i, p, rows=PART, k=0):
        n, r = len(peers), pl.ds(pl.multiple_of(row_at(step, i, p) + k * SHARE, SHARE), rows)
        peers.append(remote(dx.at[r, mine], dx.at[r, mine], peer_send.at[n], peer_recv.at[n], peer))
        peers[-1].start()

    def own_block(i):
        for p in range(2):
            for q in range(PIECES):
                total = summed(6 + i, own_rows(i), i, q, p)
                for side in range(2):
                    k = p if side == 1 else 1 - p
                    near_copy(i, k, side, q).wait_recv()
                    total += near[side, i, k, q].astype(jnp.float32)
                dx[pl.ds(row_at(0, i, p), PART), cols_of(core, q)] = total.astype(dx.dtype)
            direct(i, p, p).start()
        direct(i, 1, 0).start()
        direct(i, 0, 1).start()
        share(0, i, 0, BLOCK)

    def weight_tiles(lo, hi):
        @pl.loop(lo, hi)
        def _(t):
            cols = pl.ds(pl.multiple_of(t * TILE, TILE), TILE)
            dw[cols, :] = dot(x[:, cols], gu[...], (0, 0)).astype(dw.dtype)

    def relay(i):
        for side in range(2):
            direct(i, side, side).wait_recv()
            for k in range(PART // SHARE):
                forward(i, side, k).start()
            share(steps[1 - side], i, side)

    def keep(i):
        for side in range(2):
            direct(i, 1 - side, side).wait_recv()
            share(steps[1 - side], i, 1 - side)

    def last(i):
        for k in range(PART // SHARE):
            for side in range(2):
                forward(i, side, k).wait_recv()
                share(2, i, side, SHARE, k)

    own_block(0)
    for b in range(8):
        x_copy(b).wait()
    weight_tiles(0, 5)
    own_block(1)
    weight_tiles(5, d // TILE)
    relay(0)
    keep(0)
    relay(1)
    keep(1)
    last(0)
    last(1)

    for i in range(2):
        stage_free(i)
        for p in range(2):
            for q in range(PIECES):
                far_copy(i, p, q).wait_send()
                for k in range(2):
                    near_copy(i, k, p, q).wait_send()
            for side in range(2):
                direct(i, p, side).wait_send()
        for side in range(2):
            for k in range(PART // SHARE):
                forward(i, side, k).wait_send()
    for c in peers:
        c.wait()


def write_kernel(dx, dw, dwd, dx_hbm, dwg_hbm, dwu_hbm, dwd_hbm, sem):
    f = dwd.shape[0]
    copies = [
        pltpu.make_async_copy(dx, dx_hbm, sem.at[0]),
        pltpu.make_async_copy(dw.at[:, pl.ds(0, f)], dwg_hbm, sem.at[1]),
        pltpu.make_async_copy(dw.at[:, pl.ds(f, f)], dwu_hbm, sem.at[2]),
        pltpu.make_async_copy(dwd, dwd_hbm, sem.at[3]),
    ]
    for c in copies:
        c.start()
    for c in copies:
        c.wait()


def solution(mesh):
    assert mesh.shape["tp"] == 2 * CHIPS

    def step(x, dy, gate, up, w_gate, w_up, w_down):
        tokens, d = x.shape
        f = w_down.shape[0]
        assert tokens == CHIPS * 2 * BLOCK
        half = d // 2
        bf16, f32 = jnp.bfloat16, jnp.float32
        dma = pltpu.SemaphoreType.DMA
        vmem, hbm = pl.BlockSpec(memory_space=pltpu.VMEM), pl.BlockSpec(memory_space=pltpu.HBM)
        dx, dw, dwd = pl.pallas_call(
            main_kernel,
            name="block_grads",
            out_shape=(pltpu.VMEM((tokens, d), bf16), pltpu.VMEM((d, 2 * f), bf16), pltpu.VMEM((f, d), bf16)),
            in_specs=[hbm] * 7,
            out_specs=(vmem,) * 3,
            scratch_shapes=[
                pltpu.VMEM((tokens, d), bf16),
                pltpu.VMEM((tokens, d), bf16),
                pltpu.VMEM((tokens, 2 * f), bf16),
                pltpu.VMEM((d, 2 * f), bf16),
                pltpu.VMEM((f, d), bf16),
                pltpu.VMEM((BLOCK, f), bf16),
                pltpu.VMEM((f, tokens), bf16),
                pltpu.VMEM((BLOCK, f), f32),
                pltpu.VMEM((2, PIECES, BLOCK, half // PIECES), f32),
                pltpu.VMEM((2, PIECES, BLOCK, half // PIECES), bf16),
                pltpu.VMEM((6, 2, PIECES, PART, half // PIECES), bf16),
                pltpu.VMEM((2, 2, PIECES, PART, half // PIECES), bf16),
                pltpu.VMEM((2, 2, 2, PIECES, PART, half // PIECES), bf16),
                dma((3,)),
                dma((3, 8, 2)),
                dma((8,)),
                dma((2, PIECES, 2)),
                dma((8, PIECES, 2)),
                dma((6, 2, PIECES)),
                dma((2, 2, PIECES)),
                dma((2, 2, 2, PIECES)),
                dma((2, 2, 2)),
                dma((2, 2, 2)),
                dma((2, 2, PART // SHARE)),
                dma((2, 2, PART // SHARE)),
                dma((10 + 4 * PART // SHARE,)),
                dma((10 + 4 * PART // SHARE,)),
            ],
            compiler_params=pltpu.CompilerParams(collective_id=0, has_side_effects=True, vmem_limit_bytes=47 * 2**20),
        )(x, dy, gate, up, w_gate, w_up, w_down)
        return pl.pallas_call(
            write_kernel,
            name="write_out",
            out_shape=tuple(
                jax.ShapeDtypeStruct(s, bf16) for s in ((tokens, d), (d, f), (d, f), (f, d))
            ),
            in_specs=[vmem] * 3,
            out_specs=(hbm,) * 4,
            scratch_shapes=[dma((4,))],
            compiler_params=pltpu.CompilerParams(vmem_limit_bytes=20 * 2**20),
        )(dx, dw, dwd)

    tokens, columns, rows = P("dp", None), P(None, "tp"), P("tp", None)
    return jax.shard_map(
        step,
        mesh=mesh,
        in_specs=(tokens, tokens, P("dp", "tp"), P("dp", "tp"), columns, columns, rows),
        out_specs=(tokens, P("dp", "tp"), P("dp", "tp"), P(("dp", "tp"), None)),
        check_vma=False,
    )
```

```python
import functools

import jax
import jax.numpy as jnp
from jax import lax
from jax.experimental import pallas as pl
from jax.experimental.pallas import tpu as pltpu
from jax.sharding import PartitionSpec as P

MESH = pl.DeviceIdType.MESH
CHIPS = 4
BLOCK = 256
PART = BLOCK // 2
PIECES = 2
SHARE = 32
STRIP = 32
TILE = 256


def act(gate, up):
    return jax.nn.gelu(gate) * up


def dot(a, b, contract):
    return lax.dot_general(a, b, ((contract[:1], contract[1:]), ((), ())), preferred_element_type=jnp.float32)


def main_kernel(
    x_hbm, dy_hbm, gate_hbm, up_hbm, wg_hbm, wu_hbm, wd_hbm,
    dx, dw, dwd,
    x, dy, gu, w, wd, hid, hid_t, dh, own, stage, sendbuf, far, near,
    in_sem, row_sem, term_send, term_recv, rs_send, far_recv, near_recv,
    ag_send, ag_recv, fwd_send, fwd_recv, peer_send, peer_recv,
):
    tokens, d = x.shape
    f = wd.shape[0]
    half = d // 2
    chunk_rows = tokens // CHIPS
    width = half // PIECES
    me = lax.axis_index("tp")
    chip, core = lax.div(me, 2), lax.rem(me, 2)
    peer = chip * 2 + 1 - core
    mine = pl.ds(pl.multiple_of(core * half, half), half)

    def chip_at(step):
        return lax.rem(chip + step, CHIPS)

    def device_at(step):
        return chip_at(step) * 2 + core

    steps = (1, CHIPS - 1)

    barrier = pltpu.get_barrier_semaphore()
    for other in (device_at(1), device_at(CHIPS - 1), peer):
        pl.semaphore_signal(barrier, inc=1, device_id={"tp": other}, device_id_type=MESH)

    def remote(src, dst, send, recv, device):
        return pltpu.make_async_remote_copy(
            src_ref=src, dst_ref=dst, send_sem=send, recv_sem=recv, device_id={"tp": device}, device_id_type=MESH
        )

    def row_at(step, i, p=0):
        return pl.multiple_of(chip_at(step) * chunk_rows + i * BLOCK + p * PART, PART)

    def row_copies(b, step, i):
        r = pl.ds(row_at(step, i), BLOCK)
        return (
            pltpu.make_async_copy(dy_hbm.at[r], dy.at[r], row_sem.at[0, b]),
            pltpu.make_async_copy(gate_hbm.at[r], gu.at[r, pl.ds(0, f)], row_sem.at[1, b]),
            pltpu.make_async_copy(up_hbm.at[r], gu.at[r, pl.ds(f, f)], row_sem.at[2, b]),
        )

    def start_rows(b, step, i):
        for c in row_copies(b, step, i):
            c.start()

    def x_copy(b):
        r = pl.ds(pl.multiple_of(b * BLOCK, BLOCK), BLOCK)
        return pltpu.make_async_copy(x_hbm.at[r], x.at[r], row_sem.at[3, b])

    in_wd = pltpu.make_async_copy(wd_hbm, wd, in_sem.at[0])
    in_wg = pltpu.make_async_copy(wg_hbm, w.at[:, pl.ds(0, f)], in_sem.at[1])
    in_wu = pltpu.make_async_copy(wu_hbm, w.at[:, pl.ds(f, f)], in_sem.at[2])
    in_wd.start()
    start_rows(0, 2, 0)
    in_wg.start()
    in_wu.start()
    start_rows(1, 2, 1)

    def hidden_block(b, step, i):
        start = row_at(step, i)
        for c in row_copies(b, step, i):
            c.wait()
        dh[...] = dot(dy[pl.ds(start, BLOCK), :], wd[...], (1, 1))

        @pl.loop(0, BLOCK // STRIP)
        def _(s):
            here = pl.ds(pl.multiple_of(s * STRIP, STRIP), STRIP)
            r = pl.ds(pl.multiple_of(start + s * STRIP, STRIP), STRIP)
            h, back = jax.vjp(act, gu[r, pl.ds(0, f)].astype(jnp.float32), gu[r, pl.ds(f, f)].astype(jnp.float32))
            d_gate, d_up = back(dh[here, :])
            gu[r, pl.ds(0, f)] = d_gate.astype(gu.dtype)
            gu[r, pl.ds(f, f)] = d_up.astype(gu.dtype)
            hid[here, :] = h.astype(hid.dtype)

        hid_t[:, pl.ds(pl.multiple_of(start, BLOCK), BLOCK)] = hid[...].T

    def cols_of(c, q):
        return pl.ds(pl.multiple_of(c * half + q * width, width), width)

    def term_copy(b, step, i, slot, q):
        rows = pl.ds(row_at(step, i), BLOCK)
        return remote(
            stage.at[slot, q], dx.at[rows, cols_of(1 - core, q)], term_send.at[slot, q], term_recv.at[b, q], peer
        )

    def term_other(b, step, i, slot):
        rows = pl.ds(row_at(step, i), BLOCK)
        for q in range(PIECES):
            stage[slot, q] = dot(gu[rows, :], w[cols_of(1 - core, q), :], (1, 1)).astype(stage.dtype)
            term_copy(b, step, i, slot, q).start()

    def term_own(step, i, slot):
        rows = pl.ds(row_at(step, i), BLOCK)
        for q in range(PIECES):
            own[slot, q] = dot(gu[rows, :], w[cols_of(core, q), :], (1, 1))

    def stage_free(slot):
        for q in range(PIECES):
            term_copy(0, 0, 0, slot, q).wait_send()

    def summed(step, i, p, q, slot):
        r = pl.ds(row_at(step, i, p), PART)
        mine_here = own[slot, q, pl.ds(pl.multiple_of(p * PART, PART), PART), :]
        return mine_here + dx[r, cols_of(core, q)].astype(jnp.float32)

    def far_copy(i, side, q):
        return remote(
            sendbuf.at[i, side, q],
            far.at[side, i, q],
            rs_send.at[i, side, q],
            far_recv.at[side, i, q],
            device_at(steps[side]),
        )

    def near_copy(j, i, p, q, side, step):
        return remote(
            sendbuf.at[2 + j, p, q],
            near.at[side, i, p, q],
            rs_send.at[2 + j, p, q],
            near_recv.at[side, i, p, q],
            device_at(step),
        )

    def finish_far(i):
        for q in range(PIECES):
            term_copy(i, 2, i, i, q).wait_recv()
            for p in range(2):
                sendbuf[i, p, q] = summed(2, i, p, q, i).astype(sendbuf.dtype)
                far_copy(i, p, q).start()

    in_wd.wait()

    hidden_block(0, 2, 0)
    start_rows(2, 1, 0)
    x_copy(0).start()
    in_wg.wait()
    in_wu.wait()
    pl.semaphore_wait(barrier, 3)
    term_other(0, 2, 0, 0)
    term_own(2, 0, 0)
    finish_far(0)

    hidden_block(1, 2, 1)
    start_rows(3, 3, 0)
    x_copy(1).start()
    term_other(1, 2, 1, 1)
    hidden_block(2, 1, 0)
    term_own(2, 1, 1)
    finish_far(1)

    @pl.loop(0, 2)
    def _(i):
        for side in range(2):
            b, step, plain = 2 + 2 * i + side, steps[side], 1 - side

            @pl.when(i == 0)
            def _():
                start_rows(4 + side, step, 1)

            @pl.when(i == 1)
            def _():
                start_rows(6 + side, 0, side)

            x_copy(b).start()
            stage_free(side)
            term_other(b, step, i, side)
            if side == 0:
                hidden_block(b + 1, steps[1], i)
            else:
                hidden_block(b + 1, 1 - i, 1 - i)
            term_own(step, i, side)
            for q in range(PIECES):
                term_copy(b, step, i, side, q).wait_recv()
                sendbuf[b, plain, q] = summed(step, i, plain, q, side).astype(sendbuf.dtype)
                near_copy(b - 2, i, plain, q, side, step).start()
        for q in range(PIECES):
            for side in range(2):
                b, step = 2 + 2 * i + side, steps[side]
                far_copy(i, side, q).wait_recv()
                sendbuf[b, side, q] = (
                    summed(step, i, side, q, side) + far[side, i, q].astype(jnp.float32)
                ).astype(sendbuf.dtype)
                near_copy(b - 2, i, side, q, side, step).start()

    x_copy(6).start()
    x_copy(7).start()
    stage_free(0)
    term_other(6, 0, 0, 0)
    hidden_block(7, 0, 1)
    term_own(0, 0, 0)
    stage_free(1)
    term_other(7, 0, 1, 1)
    term_own(0, 1, 1)

    def direct(i, p, side):
        r = pl.ds(row_at(0, i, p), PART)
        return remote(
            dx.at[r, mine], dx.at[r, mine], ag_send.at[side, i, p], ag_recv.at[side, i, p], device_at(steps[side])
        )

    def forward(i, side, k):
        r = pl.ds(pl.multiple_of(row_at(steps[1 - side], i, side) + k * SHARE, SHARE), SHARE)
        return remote(
            dx.at[r, mine], dx.at[r, mine], fwd_send.at[side, i, k], fwd_recv.at[side, i, k], device_at(steps[side])
        )

    peers = []

    def share(step, i, p, rows=PART, k=0):
        n, r = len(peers), pl.ds(pl.multiple_of(row_at(step, i, p) + k * SHARE, SHARE), rows)
        peers.append(remote(dx.at[r, mine], dx.at[r, mine], peer_send.at[n], peer_recv.at[n], peer))
        peers[-1].start()

    def own_block(i):
        for q in range(PIECES):
            term_copy(6 + i, 0, i, i, q).wait_recv()
        for p in range(2):
            for q in range(PIECES):
                total = summed(0, i, p, q, i)
                for side in range(2):
                    near_copy(0, i, p, q, side, 0).wait_recv()
                    total += near[side, i, p, q].astype(jnp.float32)
                dx[pl.ds(row_at(0, i, p), PART), cols_of(core, q)] = total.astype(dx.dtype)
            direct(i, p, p).start()
        direct(i, 1, 0).start()
        direct(i, 0, 1).start()
        share(0, i, 0, BLOCK)

    def down_tiles(lo, hi):
        @pl.loop(lo, hi)
        def _(t):
            cols = pl.ds(pl.multiple_of(t * (d // 4), d // 4), d // 4)
            dwd[:, cols] = dot(hid_t[...], dy[:, cols], (1, 0)).astype(dwd.dtype)

    def weight_tiles(lo, hi):
        @pl.loop(lo, hi)
        def _(t):
            cols = pl.ds(pl.multiple_of(t * TILE, TILE), TILE)
            dw[cols, :] = dot(x[:, cols], gu[...], (0, 0)).astype(dw.dtype)

    def relay(i):
        for side in range(2):
            direct(i, side, side).wait_recv()
            for k in range(PART // SHARE):
                forward(i, side, k).start()
            share(steps[1 - side], i, side)

    def keep(i):
        for side in range(2):
            direct(i, 1 - side, side).wait_recv()
            share(steps[1 - side], i, 1 - side)

    def last(i):
        for k in range(PART // SHARE):
            for side in range(2):
                forward(i, side, k).wait_recv()
                share(2, i, side, SHARE, k)

    own_block(0)
    own_block(1)
    down_tiles(0, 4)
    relay(0)
    for b in range(8):
        x_copy(b).wait()
    weight_tiles(0, 2)
    keep(0)
    weight_tiles(2, 5)
    relay(1)
    weight_tiles(5, d // TILE)
    keep(1)
    last(0)
    last(1)

    for i in range(2):
        stage_free(i)
        for p in range(2):
            for q in range(PIECES):
                far_copy(i, p, q).wait_send()
                for side in range(2):
                    near_copy(2 * i + side, i, p, q, side, steps[side]).wait_send()
            for side in range(2):
                direct(i, p, side).wait_send()
        for side in range(2):
            for k in range(PART // SHARE):
                forward(i, side, k).wait_send()
    for c in peers:
        c.wait()


def write_kernel(dx, dw, dwd, dx_hbm, dwg_hbm, dwu_hbm, dwd_hbm, sem):
    f = dwd.shape[0]
    copies = [
        pltpu.make_async_copy(dx, dx_hbm, sem.at[0]),
        pltpu.make_async_copy(dw.at[:, pl.ds(0, f)], dwg_hbm, sem.at[1]),
        pltpu.make_async_copy(dw.at[:, pl.ds(f, f)], dwu_hbm, sem.at[2]),
        pltpu.make_async_copy(dwd, dwd_hbm, sem.at[3]),
    ]
    for c in copies:
        c.start()
    for c in copies:
        c.wait()


def solution(mesh):
    assert mesh.shape["tp"] == 2 * CHIPS

    def step(x, dy, gate, up, w_gate, w_up, w_down):
        tokens, d = x.shape
        f = w_down.shape[0]
        assert tokens == CHIPS * 2 * BLOCK
        half = d // 2
        bf16, f32 = jnp.bfloat16, jnp.float32
        dma = pltpu.SemaphoreType.DMA
        vmem, hbm = pl.BlockSpec(memory_space=pltpu.VMEM), pl.BlockSpec(memory_space=pltpu.HBM)
        dx, dw, dwd = pl.pallas_call(
            main_kernel,
            name="block_grads",
            out_shape=(pltpu.VMEM((tokens, d), bf16), pltpu.VMEM((d, 2 * f), bf16), pltpu.VMEM((f, d), bf16)),
            in_specs=[hbm] * 7,
            out_specs=(vmem,) * 3,
            scratch_shapes=[
                pltpu.VMEM((tokens, d), bf16),
                pltpu.VMEM((tokens, d), bf16),
                pltpu.VMEM((tokens, 2 * f), bf16),
                pltpu.VMEM((d, 2 * f), bf16),
                pltpu.VMEM((f, d), bf16),
                pltpu.VMEM((BLOCK, f), bf16),
                pltpu.VMEM((f, tokens), bf16),
                pltpu.VMEM((BLOCK, f), f32),
                pltpu.VMEM((2, PIECES, BLOCK, half // PIECES), f32),
                pltpu.VMEM((2, PIECES, BLOCK, half // PIECES), bf16),
                pltpu.VMEM((6, 2, PIECES, PART, half // PIECES), bf16),
                pltpu.VMEM((2, 2, PIECES, PART, half // PIECES), bf16),
                pltpu.VMEM((2, 2, 2, PIECES, PART, half // PIECES), bf16),
                dma((3,)),
                dma((4, 8)),
                dma((2, PIECES)),
                dma((8, PIECES)),
                dma((6, 2, PIECES)),
                dma((2, 2, PIECES)),
                dma((2, 2, 2, PIECES)),
                dma((2, 2, 2)),
                dma((2, 2, 2)),
                dma((2, 2, PART // SHARE)),
                dma((2, 2, PART // SHARE)),
                dma((10 + 4 * PART // SHARE,)),
                dma((10 + 4 * PART // SHARE,)),
            ],
            compiler_params=pltpu.CompilerParams(collective_id=0, has_side_effects=True, vmem_limit_bytes=47 * 2**20),
        )(x, dy, gate, up, w_gate, w_up, w_down)
        return pl.pallas_call(
            write_kernel,
            name="write_out",
            out_shape=tuple(
                jax.ShapeDtypeStruct(s, bf16) for s in ((tokens, d), (d, f), (d, f), (f, d))
            ),
            in_specs=[vmem] * 3,
            out_specs=(hbm,) * 4,
            scratch_shapes=[dma((4,))],
            compiler_params=pltpu.CompilerParams(vmem_limit_bytes=20 * 2**20),
        )(dx, dw, dwd)

    tokens, columns, rows = P("dp", None), P(None, "tp"), P("tp", None)
    return jax.shard_map(
        step,
        mesh=mesh,
        in_specs=(tokens, tokens, P("dp", "tp"), P("dp", "tp"), columns, columns, rows),
        out_specs=(tokens, P("dp", "tp"), P("dp", "tp"), P(("dp", "tp"), None)),
        check_vma=False,
    )
```

```python
import functools

import jax
import jax.numpy as jnp
from jax import lax
from jax.experimental import pallas as pl
from jax.experimental.pallas import tpu as pltpu
from jax.sharding import PartitionSpec as P

MESH = pl.DeviceIdType.MESH
CHIPS = 4
BLOCK = 256
PART = BLOCK // 2
PIECES = 2
SHARE = 32
STRIP = 32
TILE = 256


def act(gate, up):
    return jax.nn.gelu(gate) * up


def dot(a, b, contract):
    return lax.dot_general(a, b, ((contract[:1], contract[1:]), ((), ())), preferred_element_type=jnp.float32)


def main_kernel(
    x_hbm, dy_hbm, gate_hbm, up_hbm, wg_hbm, wu_hbm, wd_hbm,
    dx, dw, dwd,
    x, dy, gu, w, wd, hid, hid_t, dh, own, stage, sendbuf, far, near,
    in_sem, row_sem, x_sem, term_send, term_recv, rs_send, far_recv, near_recv,
    ag_send, ag_recv, fwd_send, fwd_recv, peer_send, peer_recv,
):
    tokens, d = x.shape
    f = wd.shape[0]
    half = d // 2
    chunk_rows = tokens // CHIPS
    width = half // PIECES
    me = lax.axis_index("tp")
    chip, core = lax.div(me, 2), lax.rem(me, 2)
    peer = chip * 2 + 1 - core
    mine = pl.ds(pl.multiple_of(core * half, half), half)

    def chip_at(step):
        return lax.rem(chip + step, CHIPS)

    def device_at(step):
        return chip_at(step) * 2 + core

    steps = (1, CHIPS - 1)

    barrier = pltpu.get_barrier_semaphore()
    for other in (device_at(1), device_at(CHIPS - 1), peer):
        pl.semaphore_signal(barrier, inc=1, device_id={"tp": other}, device_id_type=MESH)

    def remote(src, dst, send, recv, device):
        return pltpu.make_async_remote_copy(
            src_ref=src, dst_ref=dst, send_sem=send, recv_sem=recv, device_id={"tp": device}, device_id_type=MESH
        )

    def row_at(step, i, p=0):
        return pl.multiple_of(chip_at(step) * chunk_rows + i * BLOCK + p * PART, PART)

    def far_runs(i):
        return ((row_at(2, i), BLOCK),)

    def near_runs(i):
        return ((row_at(1, i), BLOCK), (row_at(CHIPS - 1, i), BLOCK))

    own_runs = ((row_at(0, 0), 2 * BLOCK),)

    def row_copies(b, runs):
        copies = []
        for n, (start, rows) in enumerate(runs):
            r = pl.ds(start, rows)
            copies += [
                pltpu.make_async_copy(dy_hbm.at[r], dy.at[r], row_sem.at[0, b, n]),
                pltpu.make_async_copy(gate_hbm.at[r], gu.at[r, pl.ds(0, f)], row_sem.at[1, b, n]),
                pltpu.make_async_copy(up_hbm.at[r], gu.at[r, pl.ds(f, f)], row_sem.at[2, b, n]),
            ]
        return copies

    def start_rows(b, runs):
        for c in row_copies(b, runs):
            c.start()

    def x_copy(b):
        r = pl.ds(pl.multiple_of(b * BLOCK, BLOCK), BLOCK)
        return pltpu.make_async_copy(x_hbm.at[r], x.at[r], x_sem.at[b])

    in_wd = pltpu.make_async_copy(wd_hbm, wd, in_sem.at[0])
    in_wg = pltpu.make_async_copy(wg_hbm, w.at[:, pl.ds(0, f)], in_sem.at[1])
    in_wu = pltpu.make_async_copy(wu_hbm, w.at[:, pl.ds(f, f)], in_sem.at[2])
    in_wd.start()
    start_rows(0, far_runs(0))
    in_wg.start()
    in_wu.start()
    start_rows(1, far_runs(1))

    def gathered(ref, runs):
        parts = [ref[pl.ds(start, rows), :] for start, rows in runs]
        return parts[0] if len(parts) == 1 else jnp.concatenate(parts, axis=0)

    def offsets(runs):
        return [sum(rows for _, rows in runs[:n]) for n in range(len(runs))]

    def hidden_block(b, runs):
        for c in row_copies(b, runs):
            c.wait()
        dh[: sum(rows for _, rows in runs), :] = dot(gathered(dy, runs), wd[...], (1, 1))
        for at, (start, rows) in zip(offsets(runs), runs):

            @pl.loop(0, rows // STRIP)
            def _(s):
                here = pl.ds(pl.multiple_of(at + s * STRIP, STRIP), STRIP)
                r = pl.ds(pl.multiple_of(start + s * STRIP, STRIP), STRIP)
                h, back = jax.vjp(act, gu[r, pl.ds(0, f)].astype(jnp.float32), gu[r, pl.ds(f, f)].astype(jnp.float32))
                d_gate, d_up = back(dh[here, :])
                gu[r, pl.ds(0, f)] = d_gate.astype(gu.dtype)
                gu[r, pl.ds(f, f)] = d_up.astype(gu.dtype)
                hid[here, :] = h.astype(hid.dtype)

    def turn_hidden(runs):
        for at, (start, rows) in zip(offsets(runs), runs):
            hid_t[:, pl.ds(pl.multiple_of(start, BLOCK), rows)] = hid[at : at + rows, :].T

    def cols_of(c, q):
        return pl.ds(pl.multiple_of(c * half + q * width, width), width)

    def term_copies(b, runs, q):
        return [
            remote(
                stage.at[q, pl.ds(at, rows)],
                dx.at[pl.ds(start, rows), cols_of(1 - core, q)],
                term_send.at[b, q, n],
                term_recv.at[b, q, n],
                peer,
            )
            for n, (at, (start, rows)) in enumerate(zip(offsets(runs), runs))
        ]

    def stage_free(b, runs):
        for q in range(PIECES):
            for c in term_copies(b, runs, q):
                c.wait_send()

    def term_block(b, runs):
        n = sum(rows for _, rows in runs)
        for q in range(PIECES):
            stage[q, :n] = dot(gathered(gu, runs), w[cols_of(1 - core, q), :], (1, 1)).astype(stage.dtype)
            for c in term_copies(b, runs, q):
                c.start()
        for q in range(PIECES):
            own[q, :n] = dot(gathered(gu, runs), w[cols_of(core, q), :], (1, 1))

    def term_arrived(b, runs, q):
        for c in term_copies(b, runs, q):
            c.wait_recv()

    def summed(at, row, q):
        return own[q, at : at + PART, :] + dx[pl.ds(row, PART), cols_of(core, q)].astype(jnp.float32)

    def far_copy(i, side, q):
        return remote(
            sendbuf.at[i, side, q],
            far.at[side, i, q],
            rs_send.at[i, side, q],
            far_recv.at[side, i, q],
            device_at(steps[side]),
        )

    def near_copy(i, k, side, q):
        b = 2 + 2 * i + k
        return remote(
            sendbuf.at[b, side, q],
            near.at[side, i, k, q],
            rs_send.at[b, side, q],
            near_recv.at[side, i, k, q],
            device_at(steps[side]),
        )

    in_wd.wait()

    @pl.loop(0, 2)
    def _(i):
        runs = far_runs(i)
        hidden_block(i, runs)
        start_rows(2 + i, near_runs(i))
        x_copy(i).start()

        @pl.when(i == 0)
        def _():
            in_wg.wait()
            in_wu.wait()
            pl.semaphore_wait(barrier, 3)

        @pl.when(i == 1)
        def _():
            stage_free(0, far_runs(0))

        term_block(i, runs)
        turn_hidden(runs)
        for q in range(PIECES):
            term_arrived(i, runs, q)
            for side in range(2):
                sendbuf[i, side, q] = summed(side * PART, row_at(2, i, side), q).astype(sendbuf.dtype)
                far_copy(i, side, q).start()

    stage_free(1, far_runs(1))
    start_rows(4, own_runs)

    @pl.loop(0, 2)
    def _(i):
        runs = near_runs(i)
        hidden_block(2 + i, runs)
        for n in range(2):
            x_copy(2 + 2 * i + n).start()

        @pl.when(i == 1)
        def _():
            stage_free(2, near_runs(0))

        term_block(2 + i, runs)
        turn_hidden(runs)
        for k in range(2):
            for q in range(PIECES):
                if k == 0:
                    term_arrived(2 + i, runs, q)
                for side in range(2):
                    p = side if k == 1 else 1 - side
                    total = summed(side * BLOCK + p * PART, row_at(steps[side], i, p), q)
                    if k == 1:
                        far_copy(i, side, q).wait_recv()
                        total += far[side, i, q].astype(jnp.float32)
                    sendbuf[2 + 2 * i + k, side, q] = total.astype(sendbuf.dtype)
                    near_copy(i, k, side, q).start()

    x_copy(6).start()
    x_copy(7).start()
    hidden_block(4, own_runs)
    stage_free(3, near_runs(1))
    term_block(4, own_runs)
    turn_hidden(own_runs)

    def direct(i, p, side):
        r = pl.ds(row_at(0, i, p), PART)
        return remote(
            dx.at[r, mine], dx.at[r, mine], ag_send.at[side, i, p], ag_recv.at[side, i, p], device_at(steps[side])
        )

    def forward(i, side, k):
        r = pl.ds(pl.multiple_of(row_at(steps[1 - side], i, side) + k * SHARE, SHARE), SHARE)
        return remote(
            dx.at[r, mine], dx.at[r, mine], fwd_send.at[side, i, k], fwd_recv.at[side, i, k], device_at(steps[side])
        )

    peers = []

    def share(step, i, p, rows=PART, k=0):
        n, r = len(peers), pl.ds(pl.multiple_of(row_at(step, i, p) + k * SHARE, SHARE), rows)
        peers.append(remote(dx.at[r, mine], dx.at[r, mine], peer_send.at[n], peer_recv.at[n], peer))
        peers[-1].start()

    def own_block(i):
        for p in range(2):
            for q in range(PIECES):
                total = summed(i * BLOCK + p * PART, row_at(0, i, p), q)
                for side in range(2):
                    k = p if side == 1 else 1 - p
                    near_copy(i, k, side, q).wait_recv()
                    total += near[side, i, k, q].astype(jnp.float32)
                dx[pl.ds(row_at(0, i, p), PART), cols_of(core, q)] = total.astype(dx.dtype)
            direct(i, p, p).start()
        direct(i, 1, 0).start()
        direct(i, 0, 1).start()
        share(0, i, 0, BLOCK)

    def down_tiles(lo, hi):
        @pl.loop(lo, hi)
        def _(t):
            cols = pl.ds(pl.multiple_of(t * (d // 4), d // 4), d // 4)
            dwd[:, cols] = dot(hid_t[...], dy[:, cols], (1, 0)).astype(dwd.dtype)

    def weight_tiles(lo, hi):
        @pl.loop(lo, hi)
        def _(t):
            cols = pl.ds(pl.multiple_of(t * TILE, TILE), TILE)
            dw[cols, :] = dot(x[:, cols], gu[...], (0, 0)).astype(dw.dtype)

    def relay(i):
        for side in range(2):
            direct(i, side, side).wait_recv()
            for k in range(PART // SHARE):
                forward(i, side, k).start()
            share(steps[1 - side], i, side)

    def keep(i):
        for side in range(2):
            direct(i, 1 - side, side).wait_recv()
            share(steps[1 - side], i, 1 - side)

    def last(i):
        for k in range(PART // SHARE):
            for side in range(2):
                forward(i, side, k).wait_recv()
                share(2, i, side, SHARE, k)

    down_tiles(0, 2)
    for q in range(PIECES):
        term_arrived(4, own_runs, q)
    own_block(0)
    for b in range(8):
        x_copy(b).wait()
    down_tiles(2, 4)
    weight_tiles(0, 2)
    own_block(1)
    weight_tiles(2, 4)
    relay(0)
    weight_tiles(4, 6)
    keep(0)
    weight_tiles(6, d // TILE)
    relay(1)
    keep(1)
    last(0)
    last(1)

    stage_free(4, own_runs)
    for i in range(2):
        for side in range(2):
            for q in range(PIECES):
                far_copy(i, side, q).wait_send()
                for k in range(2):
                    near_copy(i, k, side, q).wait_send()
            for p in range(2):
                direct(i, p, side).wait_send()
            for k in range(PART // SHARE):
                forward(i, side, k).wait_send()
    for c in peers:
        c.wait()


def write_kernel(dx, dw, dwd, dx_hbm, dwg_hbm, dwu_hbm, dwd_hbm, sem):
    f = dwd.shape[0]
    copies = [
        pltpu.make_async_copy(dx, dx_hbm, sem.at[0]),
        pltpu.make_async_copy(dw.at[:, pl.ds(0, f)], dwg_hbm, sem.at[1]),
        pltpu.make_async_copy(dw.at[:, pl.ds(f, f)], dwu_hbm, sem.at[2]),
        pltpu.make_async_copy(dwd, dwd_hbm, sem.at[3]),
    ]
    for c in copies:
        c.start()
    for c in copies:
        c.wait()


def solution(mesh):
    assert mesh.shape["tp"] == 2 * CHIPS

    def step(x, dy, gate, up, w_gate, w_up, w_down):
        tokens, d = x.shape
        f = w_down.shape[0]
        assert tokens == CHIPS * 2 * BLOCK
        half = d // 2
        bf16, f32 = jnp.bfloat16, jnp.float32
        dma = pltpu.SemaphoreType.DMA
        vmem, hbm = pl.BlockSpec(memory_space=pltpu.VMEM), pl.BlockSpec(memory_space=pltpu.HBM)
        dx, dw, dwd = pl.pallas_call(
            main_kernel,
            name="block_grads",
            out_shape=(pltpu.VMEM((tokens, d), bf16), pltpu.VMEM((d, 2 * f), bf16), pltpu.VMEM((f, d), bf16)),
            in_specs=[hbm] * 7,
            out_specs=(vmem,) * 3,
            scratch_shapes=[
                pltpu.VMEM((tokens, d), bf16),
                pltpu.VMEM((tokens, d), bf16),
                pltpu.VMEM((tokens, 2 * f), bf16),
                pltpu.VMEM((d, 2 * f), bf16),
                pltpu.VMEM((f, d), bf16),
                pltpu.VMEM((2 * BLOCK, f), bf16),
                pltpu.VMEM((f, tokens), bf16),
                pltpu.VMEM((2 * BLOCK, f), f32),
                pltpu.VMEM((PIECES, 2 * BLOCK, half // PIECES), f32),
                pltpu.VMEM((PIECES, 2 * BLOCK, half // PIECES), bf16),
                pltpu.VMEM((6, 2, PIECES, PART, half // PIECES), bf16),
                pltpu.VMEM((2, 2, PIECES, PART, half // PIECES), bf16),
                pltpu.VMEM((2, 2, 2, PIECES, PART, half // PIECES), bf16),
                dma((3,)),
                dma((3, 5, 2)),
                dma((8,)),
                dma((5, PIECES, 2)),
                dma((5, PIECES, 2)),
                dma((6, 2, PIECES)),
                dma((2, 2, PIECES)),
                dma((2, 2, 2, PIECES)),
                dma((2, 2, 2)),
                dma((2, 2, 2)),
                dma((2, 2, PART // SHARE)),
                dma((2, 2, PART // SHARE)),
                dma((10 + 4 * PART // SHARE,)),
                dma((10 + 4 * PART // SHARE,)),
            ],
            compiler_params=pltpu.CompilerParams(collective_id=0, has_side_effects=True, vmem_limit_bytes=47 * 2**20),
        )(x, dy, gate, up, w_gate, w_up, w_down)
        return pl.pallas_call(
            write_kernel,
            name="write_out",
            out_shape=tuple(
                jax.ShapeDtypeStruct(s, bf16) for s in ((tokens, d), (d, f), (d, f), (f, d))
            ),
            in_specs=[vmem] * 3,
            out_specs=(hbm,) * 4,
            scratch_shapes=[dma((4,))],
            compiler_params=pltpu.CompilerParams(vmem_limit_bytes=20 * 2**20),
        )(dx, dw, dwd)

    tokens, columns, rows = P("dp", None), P(None, "tp"), P("tp", None)
    return jax.shard_map(
        step,
        mesh=mesh,
        in_specs=(tokens, tokens, P("dp", "tp"), P("dp", "tp"), columns, columns, rows),
        out_specs=(tokens, P("dp", "tp"), P("dp", "tp"), P(("dp", "tp"), None)),
        check_vma=False,
    )
```

```python
import functools

import jax
import jax.numpy as jnp
from jax import lax
from jax.experimental import pallas as pl
from jax.experimental.pallas import tpu as pltpu
from jax.sharding import PartitionSpec as P

MESH = pl.DeviceIdType.MESH
CHIPS = 4
BLOCK = 256
PART = BLOCK // 2
PIECES = 2
NARROW = 256
SHARE = 32
STRIP = 32
TILE = 256


def act(gate, up):
    return jax.nn.gelu(gate) * up


def dot(a, b, contract):
    return lax.dot_general(a, b, ((contract[:1], contract[1:]), ((), ())), preferred_element_type=jnp.float32)


def main_kernel(
    x_hbm, dy_hbm, gate_hbm, up_hbm, wg_hbm, wu_hbm, wd_hbm,
    dx, dw, dwd,
    x, dy, gu, w, wd, hid, hid_t, dh, own, stage, sendbuf, far, near,
    first_sem, row_sem, x_sem, term_send, term_recv, rs_send, far_recv, near_recv,
    ag_send, ag_recv, fwd_send, fwd_recv, peer_send, peer_recv, first_send, first_recv,
):
    tokens, d = x.shape
    f = wd.shape[0]
    half = d // 2
    chunk_rows = tokens // CHIPS
    width = half // PIECES
    me = lax.axis_index("tp")
    chip, core = lax.div(me, 2), lax.rem(me, 2)
    peer = chip * 2 + 1 - core
    mine = pl.ds(pl.multiple_of(core * half, half), half)

    def chip_at(step):
        return lax.rem(chip + step, CHIPS)

    def device_at(step):
        return chip_at(step) * 2 + core

    steps = (1, CHIPS - 1)

    barrier = pltpu.get_barrier_semaphore()
    for other in (device_at(1), device_at(CHIPS - 1), peer):
        pl.semaphore_signal(barrier, inc=1, device_id={"tp": other}, device_id_type=MESH)

    def remote(src, dst, send, recv, device):
        return pltpu.make_async_remote_copy(
            src_ref=src, dst_ref=dst, send_sem=send, recv_sem=recv, device_id={"tp": device}, device_id_type=MESH
        )

    def row_at(step, i, p=0):
        return pl.multiple_of(chip_at(step) * chunk_rows + i * BLOCK + p * PART, PART)

    def far_runs(i):
        return ((row_at(2, i), BLOCK),)

    def near_runs(i):
        return ((row_at(1, i), BLOCK), (row_at(CHIPS - 1, i), BLOCK))

    own_runs = ((row_at(0, 0), 2 * BLOCK),)

    def row_copies(b, runs):
        copies = []
        for n, (start, rows) in enumerate(runs):
            r = pl.ds(start, rows)
            copies += [
                pltpu.make_async_copy(dy_hbm.at[r], dy.at[r], row_sem.at[0, b, n]),
                pltpu.make_async_copy(gate_hbm.at[r], gu.at[r, pl.ds(0, f)], row_sem.at[1, b, n]),
                pltpu.make_async_copy(up_hbm.at[r], gu.at[r, pl.ds(f, f)], row_sem.at[2, b, n]),
            ]
        return copies

    def start_rows(b, runs):
        for c in row_copies(b, runs):
            c.start()

    def x_copy(b):
        r = pl.ds(pl.multiple_of(b * BLOCK, BLOCK), BLOCK)
        return pltpu.make_async_copy(x_hbm.at[r], x.at[r], x_sem.at[b])

    first_rows = pl.ds(row_at(2, 0), BLOCK)

    def first_copies(h):
        cols = pl.ds(h * half, half)
        return (
            pltpu.make_async_copy(dy_hbm.at[first_rows, cols], dy.at[first_rows, cols], first_sem.at[0, h]),
            pltpu.make_async_copy(wd_hbm.at[:, cols], wd.at[:, cols], first_sem.at[1, h]),
        )

    def w_copies(n, c):
        r = pl.ds(pl.multiple_of(c * half, half), half)
        return (
            pltpu.make_async_copy(wg_hbm.at[r], w.at[r, pl.ds(0, f)], first_sem.at[2, n]),
            pltpu.make_async_copy(wu_hbm.at[r], w.at[r, pl.ds(f, f)], first_sem.at[3, n]),
        )

    for h in range(2):
        for c in first_copies(h):
            c.start()
    for c in row_copies(0, far_runs(0))[1:]:
        c.start()
    for n, c in enumerate((1 - core, core)):
        for each in w_copies(n, c):
            each.start()
    start_rows(1, far_runs(1))

    def gathered(ref, runs):
        parts = [ref[pl.ds(start, rows), :] for start, rows in runs]
        return parts[0] if len(parts) == 1 else jnp.concatenate(parts, axis=0)

    def offsets(runs):
        return [sum(rows for _, rows in runs[:n]) for n in range(len(runs))]

    def hidden_block(b, runs):
        for c in row_copies(b, runs):
            c.wait()
        dh[: sum(rows for _, rows in runs), :] = dot(gathered(dy, runs), wd[...], (1, 1))
        through_act(runs)

    def through_act(runs):
        for at, (start, rows) in zip(offsets(runs), runs):

            @pl.loop(0, rows // STRIP)
            def _(s):
                here = pl.ds(pl.multiple_of(at + s * STRIP, STRIP), STRIP)
                r = pl.ds(pl.multiple_of(start + s * STRIP, STRIP), STRIP)
                h, back = jax.vjp(act, gu[r, pl.ds(0, f)].astype(jnp.float32), gu[r, pl.ds(f, f)].astype(jnp.float32))
                d_gate, d_up = back(dh[here, :])
                gu[r, pl.ds(0, f)] = d_gate.astype(gu.dtype)
                gu[r, pl.ds(f, f)] = d_up.astype(gu.dtype)
                hid[here, :] = h.astype(hid.dtype)

    def turn_hidden(runs):
        for at, (start, rows) in zip(offsets(runs), runs):
            hid_t[:, pl.ds(pl.multiple_of(start, BLOCK), rows)] = hid[at : at + rows, :].T

    def cols_of(c, q):
        return pl.ds(pl.multiple_of(c * half + q * width, width), width)

    def term_copies(b, runs, q):
        return [
            remote(
                stage.at[q, pl.ds(at, rows)],
                dx.at[pl.ds(start, rows), cols_of(1 - core, q)],
                term_send.at[b, q, n],
                term_recv.at[b, q, n],
                peer,
            )
            for n, (at, (start, rows)) in enumerate(zip(offsets(runs), runs))
        ]

    def stage_free(b, runs):
        for q in range(PIECES):
            for c in term_copies(b, runs, q):
                c.wait_send()

    def term_block(b, runs):
        n = sum(rows for _, rows in runs)
        for q in range(PIECES):
            stage[q, :n] = dot(gathered(gu, runs), w[cols_of(1 - core, q), :], (1, 1)).astype(stage.dtype)
            for c in term_copies(b, runs, q):
                c.start()
        for q in range(PIECES):
            own[q, :n] = dot(gathered(gu, runs), w[cols_of(core, q), :], (1, 1))

    def term_arrived(b, runs, q):
        for c in term_copies(b, runs, q):
            c.wait_recv()

    def summed(at, row, q):
        return own[q, at : at + PART, :] + dx[pl.ds(row, PART), cols_of(core, q)].astype(jnp.float32)

    def far_copy(i, side, q):
        return remote(
            sendbuf.at[i, side, q],
            far.at[side, i, q],
            rs_send.at[i, side, q],
            far_recv.at[side, i, q],
            device_at(steps[side]),
        )

    def near_copy(i, k, side, q):
        b = 2 + 2 * i + k
        return remote(
            sendbuf.at[b, side, q],
            near.at[side, i, k, q],
            rs_send.at[b, side, q],
            near_recv.at[side, i, k, q],
            device_at(steps[side]),
        )

    def first_term(v):
        cols = pl.ds(pl.multiple_of((1 - core) * half + v * NARROW, NARROW), NARROW)
        q, here = v * NARROW // width, pl.ds(v * NARROW % width, NARROW)
        return remote(
            stage.at[q, pl.ds(0, BLOCK), here],
            dx.at[first_rows, cols],
            first_send.at[v],
            first_recv.at[v],
            peer,
        )

    def first_part(v, side):
        q, here = v * NARROW // width, pl.ds(v * NARROW % width, NARROW)
        return remote(
            sendbuf.at[0, side, q, :, here],
            far.at[side, 0, q, :, here],
            rs_send.at[0, side, q],
            far_recv.at[side, 0, q],
            device_at(steps[side]),
        )

    for h in range(2):
        for c in first_copies(h):
            c.wait()
        part = dot(dy[first_rows, h * half : (h + 1) * half], wd[:, h * half : (h + 1) * half], (1, 1))
        dh[:BLOCK, :] = part if h == 0 else dh[:BLOCK, :] + part
    for c in row_copies(0, far_runs(0))[1:]:
        c.wait()
    through_act(far_runs(0))
    for c in w_copies(0, 1 - core):
        c.wait()
    pl.semaphore_wait(barrier, 3)
    for v in range(half // NARROW):
        q, here = v * NARROW // width, slice(v * NARROW % width, v * NARROW % width + NARROW)
        cols = pl.ds(pl.multiple_of((1 - core) * half + v * NARROW, NARROW), NARROW)
        stage[q, :BLOCK, here] = dot(gu[first_rows, :], w[cols, :], (1, 1)).astype(stage.dtype)
        first_term(v).start()
    for c in w_copies(1, core):
        c.wait()
    for v in range(half // NARROW):
        q, here = v * NARROW // width, slice(v * NARROW % width, v * NARROW % width + NARROW)
        cols = pl.ds(pl.multiple_of(core * half + v * NARROW, NARROW), NARROW)
        total = dot(gu[first_rows, :], w[cols, :], (1, 1))
        first_term(v).wait_recv()
        total += dx[first_rows, cols].astype(jnp.float32)
        for side in range(2):
            sendbuf[0, side, q, :, here] = total[side * PART : (side + 1) * PART].astype(sendbuf.dtype)
            first_part(v, side).start()
    turn_hidden(far_runs(0))
    start_rows(2, near_runs(0))
    x_copy(0).start()

    hidden_block(1, far_runs(1))
    start_rows(3, near_runs(1))
    x_copy(1).start()
    for v in range(half // NARROW):
        first_term(v).wait_send()
    term_block(1, far_runs(1))
    turn_hidden(far_runs(1))
    for q in range(PIECES):
        term_arrived(1, far_runs(1), q)
        for side in range(2):
            sendbuf[1, side, q] = summed(side * PART, row_at(2, 1, side), q).astype(sendbuf.dtype)
            far_copy(1, side, q).start()

    stage_free(1, far_runs(1))
    start_rows(4, own_runs)

    @pl.loop(0, 2)
    def _(i):
        runs = near_runs(i)
        hidden_block(2 + i, runs)
        for n in range(2):
            x_copy(2 + 2 * i + n).start()

        @pl.when(i == 1)
        def _():
            stage_free(2, near_runs(0))

        term_block(2 + i, runs)
        turn_hidden(runs)
        for k in range(2):
            for q in range(PIECES):
                if k == 0:
                    term_arrived(2 + i, runs, q)
                for side in range(2):
                    p = side if k == 1 else 1 - side
                    total = summed(side * BLOCK + p * PART, row_at(steps[side], i, p), q)
                    if k == 1:
                        far_copy(i, side, q).wait_recv()
                        total += far[side, i, q].astype(jnp.float32)
                    sendbuf[2 + 2 * i + k, side, q] = total.astype(sendbuf.dtype)
                    near_copy(i, k, side, q).start()

    x_copy(6).start()
    x_copy(7).start()
    hidden_block(4, own_runs)
    stage_free(3, near_runs(1))
    term_block(4, own_runs)
    turn_hidden(own_runs)

    def direct(i, p, side):
        r = pl.ds(row_at(0, i, p), PART)
        return remote(
            dx.at[r, mine], dx.at[r, mine], ag_send.at[side, i, p], ag_recv.at[side, i, p], device_at(steps[side])
        )

    def forward(i, side, k):
        r = pl.ds(pl.multiple_of(row_at(steps[1 - side], i, side) + k * SHARE, SHARE), SHARE)
        return remote(
            dx.at[r, mine], dx.at[r, mine], fwd_send.at[side, i, k], fwd_recv.at[side, i, k], device_at(steps[side])
        )

    peers = []

    def share(step, i, p, rows=PART, k=0):
        n, r = len(peers), pl.ds(pl.multiple_of(row_at(step, i, p) + k * SHARE, SHARE), rows)
        peers.append(remote(dx.at[r, mine], dx.at[r, mine], peer_send.at[n], peer_recv.at[n], peer))
        peers[-1].start()

    def own_block(i):
        for p in range(2):
            for q in range(PIECES):
                total = summed(i * BLOCK + p * PART, row_at(0, i, p), q)
                for side in range(2):
                    k = p if side == 1 else 1 - p
                    near_copy(i, k, side, q).wait_recv()
                    total += near[side, i, k, q].astype(jnp.float32)
                dx[pl.ds(row_at(0, i, p), PART), cols_of(core, q)] = total.astype(dx.dtype)
            direct(i, p, p).start()
        direct(i, 1, 0).start()
        direct(i, 0, 1).start()
        share(0, i, 0, BLOCK)

    def down_tiles(lo, hi):
        @pl.loop(lo, hi)
        def _(t):
            cols = pl.ds(pl.multiple_of(t * (d // 4), d // 4), d // 4)
            dwd[:, cols] = dot(hid_t[...], dy[:, cols], (1, 0)).astype(dwd.dtype)

    def weight_tiles(lo, hi):
        @pl.loop(lo, hi)
        def _(t):
            cols = pl.ds(pl.multiple_of(t * TILE, TILE), TILE)
            dw[cols, :] = dot(x[:, cols], gu[...], (0, 0)).astype(dw.dtype)

    def relay(i):
        for side in range(2):
            direct(i, side, side).wait_recv()
            for k in range(PART // SHARE):
                forward(i, side, k).start()
            share(steps[1 - side], i, side)

    def keep(i):
        for side in range(2):
            direct(i, 1 - side, side).wait_recv()
            share(steps[1 - side], i, 1 - side)

    def last(i):
        for k in range(PART // SHARE):
            for side in range(2):
                forward(i, side, k).wait_recv()
                share(2, i, side, SHARE, k)

    down_tiles(0, 2)
    for q in range(PIECES):
        term_arrived(4, own_runs, q)
    own_block(0)
    for b in range(8):
        x_copy(b).wait()
    down_tiles(2, 4)
    weight_tiles(0, 2)
    own_block(1)
    weight_tiles(2, 4)
    relay(0)
    weight_tiles(4, 6)
    keep(0)
    weight_tiles(6, d // TILE)
    relay(1)
    keep(1)
    last(0)
    last(1)

    stage_free(4, own_runs)
    for i in range(2):
        for side in range(2):
            for q in range(PIECES):
                far_copy(i, side, q).wait_send()
                for k in range(2):
                    near_copy(i, k, side, q).wait_send()
            for p in range(2):
                direct(i, p, side).wait_send()
            for k in range(PART // SHARE):
                forward(i, side, k).wait_send()
    for c in peers:
        c.wait()


def write_kernel(dx, dw, dwd, dx_hbm, dwg_hbm, dwu_hbm, dwd_hbm, sem):
    f = dwd.shape[0]
    copies = [
        pltpu.make_async_copy(dx, dx_hbm, sem.at[0]),
        pltpu.make_async_copy(dw.at[:, pl.ds(0, f)], dwg_hbm, sem.at[1]),
        pltpu.make_async_copy(dw.at[:, pl.ds(f, f)], dwu_hbm, sem.at[2]),
        pltpu.make_async_copy(dwd, dwd_hbm, sem.at[3]),
    ]
    for c in copies:
        c.start()
    for c in copies:
        c.wait()


def solution(mesh):
    assert mesh.shape["tp"] == 2 * CHIPS

    def step(x, dy, gate, up, w_gate, w_up, w_down):
        tokens, d = x.shape
        f = w_down.shape[0]
        assert tokens == CHIPS * 2 * BLOCK
        half = d // 2
        bf16, f32 = jnp.bfloat16, jnp.float32
        dma = pltpu.SemaphoreType.DMA
        vmem, hbm = pl.BlockSpec(memory_space=pltpu.VMEM), pl.BlockSpec(memory_space=pltpu.HBM)
        dx, dw, dwd = pl.pallas_call(
            main_kernel,
            name="block_grads",
            out_shape=(pltpu.VMEM((tokens, d), bf16), pltpu.VMEM((d, 2 * f), bf16), pltpu.VMEM((f, d), bf16)),
            in_specs=[hbm] * 7,
            out_specs=(vmem,) * 3,
            scratch_shapes=[
                pltpu.VMEM((tokens, d), bf16),
                pltpu.VMEM((tokens, d), bf16),
                pltpu.VMEM((tokens, 2 * f), bf16),
                pltpu.VMEM((d, 2 * f), bf16),
                pltpu.VMEM((f, d), bf16),
                pltpu.VMEM((2 * BLOCK, f), bf16),
                pltpu.VMEM((f, tokens), bf16),
                pltpu.VMEM((2 * BLOCK, f), f32),
                pltpu.VMEM((PIECES, 2 * BLOCK, half // PIECES), f32),
                pltpu.VMEM((PIECES, 2 * BLOCK, half // PIECES), bf16),
                pltpu.VMEM((6, 2, PIECES, PART, half // PIECES), bf16),
                pltpu.VMEM((2, 2, PIECES, PART, half // PIECES), bf16),
                pltpu.VMEM((2, 2, 2, PIECES, PART, half // PIECES), bf16),
                dma((4, 2)),
                dma((3, 5, 2)),
                dma((8,)),
                dma((5, PIECES, 2)),
                dma((5, PIECES, 2)),
                dma((6, 2, PIECES)),
                dma((2, 2, PIECES)),
                dma((2, 2, 2, PIECES)),
                dma((2, 2, 2)),
                dma((2, 2, 2)),
                dma((2, 2, PART // SHARE)),
                dma((2, 2, PART // SHARE)),
                dma((10 + 4 * PART // SHARE,)),
                dma((10 + 4 * PART // SHARE,)),
                dma((half // NARROW,)),
                dma((half // NARROW,)),
            ],
            compiler_params=pltpu.CompilerParams(collective_id=0, has_side_effects=True, vmem_limit_bytes=47 * 2**20),
        )(x, dy, gate, up, w_gate, w_up, w_down)
        return pl.pallas_call(
            write_kernel,
            name="write_out",
            out_shape=tuple(
                jax.ShapeDtypeStruct(s, bf16) for s in ((tokens, d), (d, f), (d, f), (f, d))
            ),
            in_specs=[vmem] * 3,
            out_specs=(hbm,) * 4,
            scratch_shapes=[dma((4,))],
            compiler_params=pltpu.CompilerParams(vmem_limit_bytes=20 * 2**20),
        )(dx, dw, dwd)

    tokens, columns, rows = P("dp", None), P(None, "tp"), P("tp", None)
    return jax.shard_map(
        step,
        mesh=mesh,
        in_specs=(tokens, tokens, P("dp", "tp"), P("dp", "tp"), columns, columns, rows),
        out_specs=(tokens, P("dp", "tp"), P("dp", "tp"), P(("dp", "tp"), None)),
        check_vma=False,
    )
```

```python
import functools

import jax
import jax.numpy as jnp
from jax import lax
from jax.experimental import pallas as pl
from jax.experimental.pallas import tpu as pltpu
from jax.sharding import PartitionSpec as P

MESH = pl.DeviceIdType.MESH
CHIPS = 4
BLOCK = 256
PART = BLOCK // 2
PIECES = 2
SHARE = 32
STRIP = 32
TILE = 256


def act(gate, up):
    return jax.nn.gelu(gate) * up


def dot(a, b, contract):
    return lax.dot_general(a, b, ((contract[:1], contract[1:]), ((), ())), preferred_element_type=jnp.float32)


def main_kernel(
    x_hbm, dy_hbm, gate_hbm, up_hbm, wg_hbm, wu_hbm, wd_hbm,
    dx, dw, dwd,
    x, dy, gu, w, wd, hid, hid_t, dh, own, stage, sendbuf, far, near,
    first_sem, row_sem, x_sem, term_send, term_recv, rs_send, far_recv, near_recv,
    ag_send, ag_recv, fwd_send, fwd_recv, peer_send, peer_recv, first_send, first_recv,
):
    tokens, d = x.shape
    f = wd.shape[0]
    half = d // 2
    chunk_rows = tokens // CHIPS
    width = half // PIECES
    me = lax.axis_index("tp")
    chip, core = lax.div(me, 2), lax.rem(me, 2)
    peer = chip * 2 + 1 - core
    mine = pl.ds(pl.multiple_of(core * half, half), half)

    def chip_at(step):
        return lax.rem(chip + step, CHIPS)

    def device_at(step):
        return chip_at(step) * 2 + core

    steps = (1, CHIPS - 1)

    barrier = pltpu.get_barrier_semaphore()
    for other in (device_at(1), device_at(CHIPS - 1), peer):
        pl.semaphore_signal(barrier, inc=1, device_id={"tp": other}, device_id_type=MESH)

    def remote(src, dst, send, recv, device):
        return pltpu.make_async_remote_copy(
            src_ref=src, dst_ref=dst, send_sem=send, recv_sem=recv, device_id={"tp": device}, device_id_type=MESH
        )

    def row_at(step, i, p=0):
        return pl.multiple_of(chip_at(step) * chunk_rows + i * BLOCK + p * PART, PART)

    def far_runs(i):
        return ((row_at(2, i), BLOCK),)

    def near_runs(i):
        return ((row_at(1, i), BLOCK), (row_at(CHIPS - 1, i), BLOCK))

    own_runs = ((row_at(0, 0), 2 * BLOCK),)

    def row_copies(b, runs):
        copies = []
        for n, (start, rows) in enumerate(runs):
            r = pl.ds(start, rows)
            copies += [
                pltpu.make_async_copy(dy_hbm.at[r], dy.at[r], row_sem.at[0, b, n]),
                pltpu.make_async_copy(gate_hbm.at[r], gu.at[r, pl.ds(0, f)], row_sem.at[1, b, n]),
                pltpu.make_async_copy(up_hbm.at[r], gu.at[r, pl.ds(f, f)], row_sem.at[2, b, n]),
            ]
        return copies

    def start_rows(b, runs):
        for c in row_copies(b, runs):
            c.start()

    def x_copy(b):
        r = pl.ds(pl.multiple_of(b * BLOCK, BLOCK), BLOCK)
        return pltpu.make_async_copy(x_hbm.at[r], x.at[r], x_sem.at[b])

    first_rows = pl.ds(row_at(2, 0), BLOCK)

    def first_copies(h):
        cols = pl.ds(h * half, half)
        return (
            pltpu.make_async_copy(dy_hbm.at[first_rows, cols], dy.at[first_rows, cols], first_sem.at[0, h]),
            pltpu.make_async_copy(wd_hbm.at[:, cols], wd.at[:, cols], first_sem.at[1, h]),
        )

    def w_copies(n, c):
        r = pl.ds(pl.multiple_of(c * half, half), half)
        return (
            pltpu.make_async_copy(wg_hbm.at[r], w.at[r, pl.ds(0, f)], first_sem.at[2, n]),
            pltpu.make_async_copy(wu_hbm.at[r], w.at[r, pl.ds(f, f)], first_sem.at[3, n]),
        )

    for h in range(2):
        for c in first_copies(h):
            c.start()
    for c in row_copies(0, far_runs(0))[1:]:
        c.start()
    for n, c in enumerate((1 - core, core)):
        for each in w_copies(n, c):
            each.start()
    start_rows(1, far_runs(1))

    def gathered(ref, runs):
        parts = [ref[pl.ds(start, rows), :] for start, rows in runs]
        return parts[0] if len(parts) == 1 else jnp.concatenate(parts, axis=0)

    def offsets(runs):
        return [sum(rows for _, rows in runs[:n]) for n in range(len(runs))]

    def hidden_block(b, runs):
        for c in row_copies(b, runs):
            c.wait()
        dh[: sum(rows for _, rows in runs), :] = dot(gathered(dy, runs), wd[...], (1, 1))
        through_act(runs)

    def through_act(runs):
        for at, (start, rows) in zip(offsets(runs), runs):

            @pl.loop(0, rows // STRIP)
            def _(s):
                here = pl.ds(pl.multiple_of(at + s * STRIP, STRIP), STRIP)
                r = pl.ds(pl.multiple_of(start + s * STRIP, STRIP), STRIP)
                h, back = jax.vjp(act, gu[r, pl.ds(0, f)].astype(jnp.float32), gu[r, pl.ds(f, f)].astype(jnp.float32))
                d_gate, d_up = back(dh[here, :])
                gu[r, pl.ds(0, f)] = d_gate.astype(gu.dtype)
                gu[r, pl.ds(f, f)] = d_up.astype(gu.dtype)
                hid[here, :] = h.astype(hid.dtype)

    def turn_hidden(runs):
        for at, (start, rows) in zip(offsets(runs), runs):
            hid_t[:, pl.ds(pl.multiple_of(start, BLOCK), rows)] = hid[at : at + rows, :].T

    def cols_of(c, q):
        return pl.ds(pl.multiple_of(c * half + q * width, width), width)

    def term_copies(b, runs, q):
        return [
            remote(
                stage.at[q, pl.ds(at, rows)],
                dx.at[pl.ds(start, rows), cols_of(1 - core, q)],
                term_send.at[b, q, n],
                term_recv.at[b, q, n],
                peer,
            )
            for n, (at, (start, rows)) in enumerate(zip(offsets(runs), runs))
        ]

    def stage_free(b, runs):
        for q in range(PIECES):
            for c in term_copies(b, runs, q):
                c.wait_send()

    def term_block(b, runs):
        n = sum(rows for _, rows in runs)
        for q in range(PIECES):
            stage[q, :n] = dot(gathered(gu, runs), w[cols_of(1 - core, q), :], (1, 1)).astype(stage.dtype)
        for q in range(PIECES):
            for c in term_copies(b, runs, q):
                c.start()
        for q in range(PIECES):
            own[q, :n] = dot(gathered(gu, runs), w[cols_of(core, q), :], (1, 1))

    def term_arrived(b, runs, q):
        for c in term_copies(b, runs, q):
            c.wait_recv()

    def summed(at, row, q):
        return own[q, at : at + PART, :] + dx[pl.ds(row, PART), cols_of(core, q)].astype(jnp.float32)

    def far_copy(i, side, q):
        return remote(
            sendbuf.at[i, side, q],
            far.at[side, i, q],
            rs_send.at[i, side, q],
            far_recv.at[side, i, q],
            device_at(steps[side]),
        )

    def near_copy(i, k, side, q):
        b = 2 + 2 * i + k
        return remote(
            sendbuf.at[b, side, q],
            near.at[side, i, k, q],
            rs_send.at[b, side, q],
            near_recv.at[side, i, k, q],
            device_at(steps[side]),
        )

    def first_term(v):
        return remote(
            stage.at[v, pl.ds(0, BLOCK)],
            dx.at[first_rows, cols_of(1 - core, v)],
            first_send.at[v],
            first_recv.at[v],
            peer,
        )

    for h in range(2):
        for c in first_copies(h):
            c.wait()
        part = dot(dy[first_rows, h * half : (h + 1) * half], wd[:, h * half : (h + 1) * half], (1, 1))
        dh[:BLOCK, :] = part if h == 0 else dh[:BLOCK, :] + part
    for c in row_copies(0, far_runs(0))[1:]:
        c.wait()
    through_act(far_runs(0))
    for c in w_copies(0, 1 - core):
        c.wait()
    pl.semaphore_wait(barrier, 3)
    for v in range(PIECES):
        stage[v, :BLOCK] = dot(gu[first_rows, :], w[cols_of(1 - core, v), :], (1, 1)).astype(stage.dtype)
        first_term(v).start()
    for c in w_copies(1, core):
        c.wait()
    for q in range(PIECES):
        own[q, :BLOCK] = dot(gu[first_rows, :], w[cols_of(core, q), :], (1, 1))
    for v in range(PIECES):
        first_term(v).wait_recv()
        for side in range(2):
            sendbuf[0, side, v] = summed(side * PART, row_at(2, 0, side), v).astype(sendbuf.dtype)
            far_copy(0, side, v).start()
    turn_hidden(far_runs(0))
    start_rows(2, near_runs(0))
    x_copy(0).start()

    hidden_block(1, far_runs(1))
    start_rows(3, near_runs(1))
    x_copy(1).start()
    for v in range(PIECES):
        first_term(v).wait_send()
    term_block(1, far_runs(1))
    turn_hidden(far_runs(1))
    for q in range(PIECES):
        term_arrived(1, far_runs(1), q)
        for side in range(2):
            sendbuf[1, side, q] = summed(side * PART, row_at(2, 1, side), q).astype(sendbuf.dtype)
            far_copy(1, side, q).start()

    stage_free(1, far_runs(1))
    start_rows(4, own_runs)

    @pl.loop(0, 2)
    def _(i):
        runs = near_runs(i)
        hidden_block(2 + i, runs)
        for n in range(2):
            x_copy(2 + 2 * i + n).start()

        @pl.when(i == 1)
        def _():
            stage_free(2, near_runs(0))

        term_block(2 + i, runs)
        turn_hidden(runs)
        for k in range(2):
            for q in range(PIECES):
                if k == 0:
                    term_arrived(2 + i, runs, q)
                for side in range(2):
                    p = side if k == 1 else 1 - side
                    total = summed(side * BLOCK + p * PART, row_at(steps[side], i, p), q)
                    if k == 1:
                        far_copy(i, side, q).wait_recv()
                        total += far[side, i, q].astype(jnp.float32)
                    sendbuf[2 + 2 * i + k, side, q] = total.astype(sendbuf.dtype)
                    near_copy(i, k, side, q).start()

    x_copy(6).start()
    x_copy(7).start()
    hidden_block(4, own_runs)
    stage_free(3, near_runs(1))
    term_block(4, own_runs)
    turn_hidden(own_runs)

    def direct(i, p, side):
        r = pl.ds(row_at(0, i, p), PART)
        return remote(
            dx.at[r, mine], dx.at[r, mine], ag_send.at[side, i, p], ag_recv.at[side, i, p], device_at(steps[side])
        )

    def forward(i, side, k):
        r = pl.ds(pl.multiple_of(row_at(steps[1 - side], i, side) + k * SHARE, SHARE), SHARE)
        return remote(
            dx.at[r, mine], dx.at[r, mine], fwd_send.at[side, i, k], fwd_recv.at[side, i, k], device_at(steps[side])
        )

    peers = []

    def share(step, i, p, rows=PART, k=0):
        n, r = len(peers), pl.ds(pl.multiple_of(row_at(step, i, p) + k * SHARE, SHARE), rows)
        peers.append(remote(dx.at[r, mine], dx.at[r, mine], peer_send.at[n], peer_recv.at[n], peer))
        peers[-1].start()

    def own_block(i):
        for p in range(2):
            for q in range(PIECES):
                total = summed(i * BLOCK + p * PART, row_at(0, i, p), q)
                for side in range(2):
                    k = p if side == 1 else 1 - p
                    near_copy(i, k, side, q).wait_recv()
                    total += near[side, i, k, q].astype(jnp.float32)
                dx[pl.ds(row_at(0, i, p), PART), cols_of(core, q)] = total.astype(dx.dtype)
            direct(i, p, p).start()
        direct(i, 1, 0).start()
        direct(i, 0, 1).start()
        share(0, i, 0, BLOCK)

    def down_tiles(lo, hi):
        @pl.loop(lo, hi)
        def _(t):
            cols = pl.ds(pl.multiple_of(t * (d // 4), d // 4), d // 4)
            dwd[:, cols] = dot(hid_t[...], dy[:, cols], (1, 0)).astype(dwd.dtype)

    def weight_tiles(lo, hi):
        @pl.loop(lo, hi)
        def _(t):
            cols = pl.ds(pl.multiple_of(t * TILE, TILE), TILE)
            dw[cols, :] = dot(x[:, cols], gu[...], (0, 0)).astype(dw.dtype)

    def relay(i):
        for side in range(2):
            direct(i, side, side).wait_recv()
            for k in range(PART // SHARE):
                forward(i, side, k).start()
            share(steps[1 - side], i, side)

    def keep(i):
        for side in range(2):
            direct(i, 1 - side, side).wait_recv()
            share(steps[1 - side], i, 1 - side)

    def last(i):
        for k in range(PART // SHARE):
            for side in range(2):
                forward(i, side, k).wait_recv()
                share(2, i, side, SHARE, k)

    down_tiles(0, 2)
    for q in range(PIECES):
        term_arrived(4, own_runs, q)
    own_block(0)
    for b in range(8):
        x_copy(b).wait()
    down_tiles(2, 4)
    weight_tiles(0, 2)
    own_block(1)
    weight_tiles(2, 4)
    relay(0)
    weight_tiles(4, 6)
    keep(0)
    weight_tiles(6, d // TILE)
    relay(1)
    keep(1)

    stage_free(4, own_runs)
    for i in range(2):
        for side in range(2):
            for q in range(PIECES):
                far_copy(i, side, q).wait_send()
                for k in range(2):
                    near_copy(i, k, side, q).wait_send()
            for p in range(2):
                direct(i, p, side).wait_send()
    done = len(peers)
    for c in peers:
        c.wait()
    last(0)
    for side in range(2):
        for k in range(PART // SHARE):
            forward(0, side, k).wait_send()
    last(1)
    for side in range(2):
        for k in range(PART // SHARE):
            forward(1, side, k).wait_send()
    for c in peers[done:]:
        c.wait()


def write_kernel(dx, dw, dwd, dx_hbm, dwg_hbm, dwu_hbm, dwd_hbm, sem):
    f = dwd.shape[0]
    copies = [
        pltpu.make_async_copy(dx, dx_hbm, sem.at[0]),
        pltpu.make_async_copy(dw.at[:, pl.ds(0, f)], dwg_hbm, sem.at[1]),
        pltpu.make_async_copy(dw.at[:, pl.ds(f, f)], dwu_hbm, sem.at[2]),
        pltpu.make_async_copy(dwd, dwd_hbm, sem.at[3]),
    ]
    for c in copies:
        c.start()
    for c in copies:
        c.wait()


def solution(mesh):
    assert mesh.shape["tp"] == 2 * CHIPS

    def step(x, dy, gate, up, w_gate, w_up, w_down):
        tokens, d = x.shape
        f = w_down.shape[0]
        assert tokens == CHIPS * 2 * BLOCK
        half = d // 2
        bf16, f32 = jnp.bfloat16, jnp.float32
        dma = pltpu.SemaphoreType.DMA
        vmem, hbm = pl.BlockSpec(memory_space=pltpu.VMEM), pl.BlockSpec(memory_space=pltpu.HBM)
        dx, dw, dwd = pl.pallas_call(
            main_kernel,
            name="block_grads",
            out_shape=(pltpu.VMEM((tokens, d), bf16), pltpu.VMEM((d, 2 * f), bf16), pltpu.VMEM((f, d), bf16)),
            in_specs=[hbm] * 7,
            out_specs=(vmem,) * 3,
            scratch_shapes=[
                pltpu.VMEM((tokens, d), bf16),
                pltpu.VMEM((tokens, d), bf16),
                pltpu.VMEM((tokens, 2 * f), bf16),
                pltpu.VMEM((d, 2 * f), bf16),
                pltpu.VMEM((f, d), bf16),
                pltpu.VMEM((2 * BLOCK, f), bf16),
                pltpu.VMEM((f, tokens), bf16),
                pltpu.VMEM((2 * BLOCK, f), f32),
                pltpu.VMEM((PIECES, 2 * BLOCK, half // PIECES), f32),
                pltpu.VMEM((PIECES, 2 * BLOCK, half // PIECES), bf16),
                pltpu.VMEM((6, 2, PIECES, PART, half // PIECES), bf16),
                pltpu.VMEM((2, 2, PIECES, PART, half // PIECES), bf16),
                pltpu.VMEM((2, 2, 2, PIECES, PART, half // PIECES), bf16),
                dma((4, 2)),
                dma((3, 5, 2)),
                dma((8,)),
                dma((5, PIECES, 2)),
                dma((5, PIECES, 2)),
                dma((6, 2, PIECES)),
                dma((2, 2, PIECES)),
                dma((2, 2, 2, PIECES)),
                dma((2, 2, 2)),
                dma((2, 2, 2)),
                dma((2, 2, PART // SHARE)),
                dma((2, 2, PART // SHARE)),
                dma((10 + 4 * PART // SHARE,)),
                dma((10 + 4 * PART // SHARE,)),
                dma((PIECES,)),
                dma((PIECES,)),
            ],
            compiler_params=pltpu.CompilerParams(collective_id=0, has_side_effects=True, vmem_limit_bytes=47 * 2**20),
        )(x, dy, gate, up, w_gate, w_up, w_down)
        return pl.pallas_call(
            write_kernel,
            name="write_out",
            out_shape=tuple(
                jax.ShapeDtypeStruct(s, bf16) for s in ((tokens, d), (d, f), (d, f), (f, d))
            ),
            in_specs=[vmem] * 3,
            out_specs=(hbm,) * 4,
            scratch_shapes=[dma((4,))],
            compiler_params=pltpu.CompilerParams(vmem_limit_bytes=20 * 2**20),
        )(dx, dw, dwd)

    tokens, columns, rows = P("dp", None), P(None, "tp"), P("tp", None)
    return jax.shard_map(
        step,
        mesh=mesh,
        in_specs=(tokens, tokens, P("dp", "tp"), P("dp", "tp"), columns, columns, rows),
        out_specs=(tokens, P("dp", "tp"), P("dp", "tp"), P(("dp", "tp"), None)),
        check_vma=False,
    )
```

```python
import functools

import jax
import jax.numpy as jnp
from jax import lax
from jax.experimental import pallas as pl
from jax.experimental.pallas import tpu as pltpu
from jax.sharding import PartitionSpec as P

MESH = pl.DeviceIdType.MESH
CHIPS = 4
BLOCK = 256
PART = BLOCK // 2
PIECES = 2
SHARE = 32
STRIP = 32
TILE = 256


def act(gate, up):
    return jax.nn.gelu(gate) * up


def dot(a, b, contract):
    return lax.dot_general(a, b, ((contract[:1], contract[1:]), ((), ())), preferred_element_type=jnp.float32)


def main_kernel(
    x_hbm, dy_hbm, gate_hbm, up_hbm, wg_hbm, wu_hbm, wd_hbm,
    dx, dw, dwd,
    x, dy, gu, w, wd, hid, hid_t, dh, own, stage, sendbuf, far, near,
    first_sem, row_sem, x_sem, term_send, term_recv, rs_send, far_recv, near_recv,
    ag_send, ag_recv, fwd_send, fwd_recv, peer_send, peer_recv, first_send, first_recv,
):
    tokens, d = x.shape
    f = wd.shape[0]
    half = d // 2
    chunk_rows = tokens // CHIPS
    width = half // PIECES
    me = lax.axis_index("tp")
    chip, core = lax.div(me, 2), lax.rem(me, 2)
    peer = chip * 2 + 1 - core
    mine = pl.ds(pl.multiple_of(core * half, half), half)

    def chip_at(step):
        return lax.rem(chip + step, CHIPS)

    def device_at(step):
        return chip_at(step) * 2 + core

    steps = (1, CHIPS - 1)

    barrier = pltpu.get_barrier_semaphore()
    for other in (device_at(1), device_at(CHIPS - 1), peer):
        pl.semaphore_signal(barrier, inc=1, device_id={"tp": other}, device_id_type=MESH)

    def remote(src, dst, send, recv, device):
        return pltpu.make_async_remote_copy(
            src_ref=src, dst_ref=dst, send_sem=send, recv_sem=recv, device_id={"tp": device}, device_id_type=MESH
        )

    def row_at(step, i, p=0):
        return pl.multiple_of(chip_at(step) * chunk_rows + i * BLOCK + p * PART, PART)

    def far_runs(i):
        return ((row_at(2, i), BLOCK),)

    def near_runs(i):
        return ((row_at(1, i), BLOCK), (row_at(CHIPS - 1, i), BLOCK))

    def sent_runs(i, k):
        return ((row_at(1, i, 1 - k), PART), (row_at(CHIPS - 1, i, k), PART))

    own_runs = ((row_at(0, 0), 2 * BLOCK),)

    def row_copies(b, runs):
        copies = []
        for n, (start, rows) in enumerate(runs):
            r = pl.ds(start, rows)
            copies += [
                pltpu.make_async_copy(dy_hbm.at[r], dy.at[r], row_sem.at[0, b, n]),
                pltpu.make_async_copy(gate_hbm.at[r], gu.at[r, pl.ds(0, f)], row_sem.at[1, b, n]),
                pltpu.make_async_copy(up_hbm.at[r], gu.at[r, pl.ds(f, f)], row_sem.at[2, b, n]),
            ]
        return copies

    def start_rows(b, runs):
        for c in row_copies(b, runs):
            c.start()

    def x_copy(b):
        r = pl.ds(pl.multiple_of(b * BLOCK, BLOCK), BLOCK)
        return pltpu.make_async_copy(x_hbm.at[r], x.at[r], x_sem.at[b])

    first_rows = pl.ds(row_at(2, 0), BLOCK)

    def first_copies(h):
        cols = pl.ds(h * half, half)
        return (
            pltpu.make_async_copy(dy_hbm.at[first_rows, cols], dy.at[first_rows, cols], first_sem.at[0, h]),
            pltpu.make_async_copy(wd_hbm.at[:, cols], wd.at[:, cols], first_sem.at[1, h]),
        )

    def w_copies(n, c):
        r = pl.ds(pl.multiple_of(c * half, half), half)
        return (
            pltpu.make_async_copy(wg_hbm.at[r], w.at[r, pl.ds(0, f)], first_sem.at[2, n]),
            pltpu.make_async_copy(wu_hbm.at[r], w.at[r, pl.ds(f, f)], first_sem.at[3, n]),
        )

    for h in range(2):
        for c in first_copies(h):
            c.start()
    for c in row_copies(0, far_runs(0))[1:]:
        c.start()
    for n, c in enumerate((1 - core, core)):
        for each in w_copies(n, c):
            each.start()
    start_rows(1, far_runs(1))

    def gathered(ref, runs):
        parts = [ref[pl.ds(start, rows), :] for start, rows in runs]
        return parts[0] if len(parts) == 1 else jnp.concatenate(parts, axis=0)

    def offsets(runs):
        return [sum(rows for _, rows in runs[:n]) for n in range(len(runs))]

    def hidden_block(b, runs):
        for c in row_copies(b, runs):
            c.wait()
        dh[: sum(rows for _, rows in runs), :] = dot(gathered(dy, runs), wd[...], (1, 1))
        through_act(runs)

    def through_act(runs):
        for at, (start, rows) in zip(offsets(runs), runs):

            @pl.loop(0, rows // STRIP)
            def _(s):
                here = pl.ds(pl.multiple_of(at + s * STRIP, STRIP), STRIP)
                r = pl.ds(pl.multiple_of(start + s * STRIP, STRIP), STRIP)
                h, back = jax.vjp(act, gu[r, pl.ds(0, f)].astype(jnp.float32), gu[r, pl.ds(f, f)].astype(jnp.float32))
                d_gate, d_up = back(dh[here, :])
                gu[r, pl.ds(0, f)] = d_gate.astype(gu.dtype)
                gu[r, pl.ds(f, f)] = d_up.astype(gu.dtype)
                hid[here, :] = h.astype(hid.dtype)

    def turn_hidden(runs):
        for at, (start, rows) in zip(offsets(runs), runs):
            hid_t[:, pl.ds(pl.multiple_of(start, BLOCK), rows)] = hid[at : at + rows, :].T

    def cols_of(c, q):
        return pl.ds(pl.multiple_of(c * half + q * width, width), width)

    def term_copies(b, runs, q, base=0):
        return [
            remote(
                stage.at[q, pl.ds(base + at, rows)],
                dx.at[pl.ds(start, rows), cols_of(1 - core, q)],
                term_send.at[b, q, n],
                term_recv.at[b, q, n],
                peer,
            )
            for n, (at, (start, rows)) in enumerate(zip(offsets(runs), runs))
        ]

    def stage_free(b, runs):
        for q in range(PIECES):
            for c in term_copies(b, runs, q):
                c.wait_send()

    def term_block(b, runs, base=0):
        n = sum(rows for _, rows in runs)
        for q in range(PIECES):
            stage[q, base : base + n] = dot(gathered(gu, runs), w[cols_of(1 - core, q), :], (1, 1)).astype(stage.dtype)
            for c in term_copies(b, runs, q, base):
                c.start()
        for q in range(PIECES):
            own[q, base : base + n] = dot(gathered(gu, runs), w[cols_of(core, q), :], (1, 1))

    def term_arrived(b, runs, q):
        for c in term_copies(b, runs, q):
            c.wait_recv()

    def summed(at, row, q):
        return own[q, at : at + PART, :] + dx[pl.ds(row, PART), cols_of(core, q)].astype(jnp.float32)

    def far_copy(i, side, q):
        return remote(
            sendbuf.at[i, side, q],
            far.at[side, i, q],
            rs_send.at[i, side, q],
            far_recv.at[side, i, q],
            device_at(steps[side]),
        )

    def near_copy(i, k, side, q):
        b = 2 + 2 * i + k
        return remote(
            sendbuf.at[b, side, q],
            near.at[side, i, k, q],
            rs_send.at[b, side, q],
            near_recv.at[side, i, k, q],
            device_at(steps[side]),
        )

    def first_term(v):
        return remote(
            stage.at[v, pl.ds(0, BLOCK)],
            dx.at[first_rows, cols_of(1 - core, v)],
            first_send.at[v],
            first_recv.at[v],
            peer,
        )

    for h in range(2):
        for c in first_copies(h):
            c.wait()
        part = dot(dy[first_rows, h * half : (h + 1) * half], wd[:, h * half : (h + 1) * half], (1, 1))
        dh[:BLOCK, :] = part if h == 0 else dh[:BLOCK, :] + part
    for c in row_copies(0, far_runs(0))[1:]:
        c.wait()
    through_act(far_runs(0))
    for c in w_copies(0, 1 - core):
        c.wait()
    pl.semaphore_wait(barrier, 3)
    for v in range(PIECES):
        stage[v, :BLOCK] = dot(gu[first_rows, :], w[cols_of(1 - core, v), :], (1, 1)).astype(stage.dtype)
        first_term(v).start()
    for c in w_copies(1, core):
        c.wait()
    for q in range(PIECES):
        own[q, :BLOCK] = dot(gu[first_rows, :], w[cols_of(core, q), :], (1, 1))
    for v in range(PIECES):
        first_term(v).wait_recv()
        for side in range(2):
            sendbuf[0, side, v] = summed(side * PART, row_at(2, 0, side), v).astype(sendbuf.dtype)
            far_copy(0, side, v).start()
    turn_hidden(far_runs(0))
    start_rows(2, near_runs(0))
    x_copy(0).start()

    hidden_block(1, far_runs(1))
    start_rows(3, near_runs(1))
    x_copy(1).start()
    for v in range(PIECES):
        first_term(v).wait_send()
    term_block(1, far_runs(1))
    turn_hidden(far_runs(1))
    for q in range(PIECES):
        term_arrived(1, far_runs(1), q)
        for side in range(2):
            sendbuf[1, side, q] = summed(side * PART, row_at(2, 1, side), q).astype(sendbuf.dtype)
            far_copy(1, side, q).start()

    stage_free(1, far_runs(1))
    start_rows(4, own_runs)

    @pl.loop(0, 2)
    def _(i):
        runs = near_runs(i)
        hidden_block(2 + i, runs)
        for n in range(2):
            x_copy(2 + 2 * i + n).start()

        @pl.when(i == 1)
        def _():
            for k in range(2):
                stage_free(2 + k, sent_runs(0, k))

        for k in range(2):
            b, sent = 2 + 2 * i + k, sent_runs(i, k)
            term_block(b, sent, k * BLOCK)
            if k == 0:
                turn_hidden(runs)
            for q in range(PIECES):
                term_arrived(b, sent, q)
                for side in range(2):
                    total = summed(k * BLOCK + side * PART, sent[side][0], q)
                    if k == 1:
                        far_copy(i, side, q).wait_recv()
                        total += far[side, i, q].astype(jnp.float32)
                    sendbuf[b, side, q] = total.astype(sendbuf.dtype)
                    near_copy(i, k, side, q).start()

    x_copy(6).start()
    x_copy(7).start()
    hidden_block(4, own_runs)
    for k in range(2):
        stage_free(4 + k, sent_runs(1, k))
    term_block(6, own_runs)
    turn_hidden(own_runs)

    def direct(i, p, side):
        r = pl.ds(row_at(0, i, p), PART)
        return remote(
            dx.at[r, mine], dx.at[r, mine], ag_send.at[side, i, p], ag_recv.at[side, i, p], device_at(steps[side])
        )

    def forward(i, side, k):
        r = pl.ds(pl.multiple_of(row_at(steps[1 - side], i, side) + k * SHARE, SHARE), SHARE)
        return remote(
            dx.at[r, mine], dx.at[r, mine], fwd_send.at[side, i, k], fwd_recv.at[side, i, k], device_at(steps[side])
        )

    peers = []

    def share(step, i, p, rows=PART, k=0):
        n, r = len(peers), pl.ds(pl.multiple_of(row_at(step, i, p) + k * SHARE, SHARE), rows)
        peers.append(remote(dx.at[r, mine], dx.at[r, mine], peer_send.at[n], peer_recv.at[n], peer))
        peers[-1].start()

    def own_block(i):
        for p in range(2):
            for q in range(PIECES):
                total = summed(i * BLOCK + p * PART, row_at(0, i, p), q)
                for side in range(2):
                    k = p if side == 1 else 1 - p
                    near_copy(i, k, side, q).wait_recv()
                    total += near[side, i, k, q].astype(jnp.float32)
                dx[pl.ds(row_at(0, i, p), PART), cols_of(core, q)] = total.astype(dx.dtype)
            direct(i, p, p).start()
        direct(i, 1, 0).start()
        direct(i, 0, 1).start()
        share(0, i, 0, BLOCK)

    def down_tiles(lo, hi):
        @pl.loop(lo, hi)
        def _(t):
            cols = pl.ds(pl.multiple_of(t * (d // 4), d // 4), d // 4)
            dwd[:, cols] = dot(hid_t[...], dy[:, cols], (1, 0)).astype(dwd.dtype)

    def weight_tiles(lo, hi):
        @pl.loop(lo, hi)
        def _(t):
            cols = pl.ds(pl.multiple_of(t * TILE, TILE), TILE)
            dw[cols, :] = dot(x[:, cols], gu[...], (0, 0)).astype(dw.dtype)

    def relay(i):
        for side in range(2):
            direct(i, side, side).wait_recv()
            for k in range(PART // SHARE):
                forward(i, side, k).start()
            share(steps[1 - side], i, side)

    def keep(i):
        for side in range(2):
            direct(i, 1 - side, side).wait_recv()
            share(steps[1 - side], i, 1 - side)

    def last(i):
        for k in range(PART // SHARE):
            for side in range(2):
                forward(i, side, k).wait_recv()
                share(2, i, side, SHARE, k)

    down_tiles(0, 2)
    for q in range(PIECES):
        term_arrived(6, own_runs, q)
    own_block(0)
    for b in range(8):
        x_copy(b).wait()
    down_tiles(2, 4)
    weight_tiles(0, 2)
    own_block(1)
    weight_tiles(2, 4)
    relay(0)
    weight_tiles(4, 6)
    keep(0)
    weight_tiles(6, d // TILE)
    relay(1)
    keep(1)

    stage_free(6, own_runs)
    for i in range(2):
        for side in range(2):
            for q in range(PIECES):
                far_copy(i, side, q).wait_send()
                for k in range(2):
                    near_copy(i, k, side, q).wait_send()
            for p in range(2):
                direct(i, p, side).wait_send()
    done = len(peers)
    for c in peers:
        c.wait()
    last(0)
    for side in range(2):
        for k in range(PART // SHARE):
            forward(0, side, k).wait_send()
    last(1)
    for side in range(2):
        for k in range(PART // SHARE):
            forward(1, side, k).wait_send()
    for c in peers[done:]:
        c.wait()


def write_kernel(dx, dw, dwd, dx_hbm, dwg_hbm, dwu_hbm, dwd_hbm, sem):
    f = dwd.shape[0]
    copies = [
        pltpu.make_async_copy(dx, dx_hbm, sem.at[0]),
        pltpu.make_async_copy(dw.at[:, pl.ds(0, f)], dwg_hbm, sem.at[1]),
        pltpu.make_async_copy(dw.at[:, pl.ds(f, f)], dwu_hbm, sem.at[2]),
        pltpu.make_async_copy(dwd, dwd_hbm, sem.at[3]),
    ]
    for c in copies:
        c.start()
    for c in copies:
        c.wait()


def solution(mesh):
    assert mesh.shape["tp"] == 2 * CHIPS

    def step(x, dy, gate, up, w_gate, w_up, w_down):
        tokens, d = x.shape
        f = w_down.shape[0]
        assert tokens == CHIPS * 2 * BLOCK
        half = d // 2
        bf16, f32 = jnp.bfloat16, jnp.float32
        dma = pltpu.SemaphoreType.DMA
        vmem, hbm = pl.BlockSpec(memory_space=pltpu.VMEM), pl.BlockSpec(memory_space=pltpu.HBM)
        dx, dw, dwd = pl.pallas_call(
            main_kernel,
            name="block_grads",
            out_shape=(pltpu.VMEM((tokens, d), bf16), pltpu.VMEM((d, 2 * f), bf16), pltpu.VMEM((f, d), bf16)),
            in_specs=[hbm] * 7,
            out_specs=(vmem,) * 3,
            scratch_shapes=[
                pltpu.VMEM((tokens, d), bf16),
                pltpu.VMEM((tokens, d), bf16),
                pltpu.VMEM((tokens, 2 * f), bf16),
                pltpu.VMEM((d, 2 * f), bf16),
                pltpu.VMEM((f, d), bf16),
                pltpu.VMEM((2 * BLOCK, f), bf16),
                pltpu.VMEM((f, tokens), bf16),
                pltpu.VMEM((2 * BLOCK, f), f32),
                pltpu.VMEM((PIECES, 2 * BLOCK, half // PIECES), f32),
                pltpu.VMEM((PIECES, 2 * BLOCK, half // PIECES), bf16),
                pltpu.VMEM((6, 2, PIECES, PART, half // PIECES), bf16),
                pltpu.VMEM((2, 2, PIECES, PART, half // PIECES), bf16),
                pltpu.VMEM((2, 2, 2, PIECES, PART, half // PIECES), bf16),
                dma((4, 2)),
                dma((3, 5, 2)),
                dma((8,)),
                dma((7, PIECES, 2)),
                dma((7, PIECES, 2)),
                dma((6, 2, PIECES)),
                dma((2, 2, PIECES)),
                dma((2, 2, 2, PIECES)),
                dma((2, 2, 2)),
                dma((2, 2, 2)),
                dma((2, 2, PART // SHARE)),
                dma((2, 2, PART // SHARE)),
                dma((10 + 4 * PART // SHARE,)),
                dma((10 + 4 * PART // SHARE,)),
                dma((PIECES,)),
                dma((PIECES,)),
            ],
            compiler_params=pltpu.CompilerParams(collective_id=0, has_side_effects=True, vmem_limit_bytes=47 * 2**20),
        )(x, dy, gate, up, w_gate, w_up, w_down)
        return pl.pallas_call(
            write_kernel,
            name="write_out",
            out_shape=tuple(
                jax.ShapeDtypeStruct(s, bf16) for s in ((tokens, d), (d, f), (d, f), (f, d))
            ),
            in_specs=[vmem] * 3,
            out_specs=(hbm,) * 4,
            scratch_shapes=[dma((4,))],
            compiler_params=pltpu.CompilerParams(vmem_limit_bytes=20 * 2**20),
        )(dx, dw, dwd)

    tokens, columns, rows = P("dp", None), P(None, "tp"), P("tp", None)
    return jax.shard_map(
        step,
        mesh=mesh,
        in_specs=(tokens, tokens, P("dp", "tp"), P("dp", "tp"), columns, columns, rows),
        out_specs=(tokens, P("dp", "tp"), P("dp", "tp"), P(("dp", "tp"), None)),
        check_vma=False,
    )
```

```python
import functools

import jax
import jax.numpy as jnp
from jax import lax
from jax.experimental import pallas as pl
from jax.experimental.pallas import tpu as pltpu
from jax.sharding import PartitionSpec as P

MESH = pl.DeviceIdType.MESH
CHIPS = 4
BLOCK = 256
PART = BLOCK // 2
PIECES = 2
SHARE = 32
STRIP = 32
TILE = 256


def act(gate, up):
    return jax.nn.gelu(gate) * up


def dot(a, b, contract):
    return lax.dot_general(a, b, ((contract[:1], contract[1:]), ((), ())), preferred_element_type=jnp.float32)


def main_kernel(
    x_hbm, dy_hbm, gate_hbm, up_hbm, wg_hbm, wu_hbm, wd_hbm,
    dx, dw, dwd,
    x, dy, gu, w, wd, hid, hid_t, dh, own, stage, sendbuf, far, near,
    first_sem, row_sem, x_sem, term_send, term_recv, rs_send, far_recv, near_recv,
    ag_send, ag_recv, fwd_send, fwd_recv, peer_send, peer_recv, first_send, first_recv,
):
    tokens, d = x.shape
    f = wd.shape[0]
    half = d // 2
    chunk_rows = tokens // CHIPS
    width = half // PIECES
    me = lax.axis_index("tp")
    chip, core = lax.div(me, 2), lax.rem(me, 2)
    peer = chip * 2 + 1 - core
    mine = pl.ds(pl.multiple_of(core * half, half), half)

    def chip_at(step):
        return lax.rem(chip + step, CHIPS)

    def device_at(step):
        return chip_at(step) * 2 + core

    steps = (1, CHIPS - 1)

    barrier = pltpu.get_barrier_semaphore()
    for other in (device_at(1), device_at(CHIPS - 1), peer):
        pl.semaphore_signal(barrier, inc=1, device_id={"tp": other}, device_id_type=MESH)

    def remote(src, dst, send, recv, device):
        return pltpu.make_async_remote_copy(
            src_ref=src, dst_ref=dst, send_sem=send, recv_sem=recv, device_id={"tp": device}, device_id_type=MESH
        )

    def row_at(step, i, p=0):
        return pl.multiple_of(chip_at(step) * chunk_rows + i * BLOCK + p * PART, PART)

    def far_runs(i):
        return ((row_at(2, i), BLOCK),)

    def sent_runs(i, k):
        return ((row_at(1, i, 1 - k), PART), (row_at(CHIPS - 1, i, k), PART))

    own_runs = ((row_at(0, 0), 2 * BLOCK),)

    def row_copies(b, runs):
        copies = []
        for n, (start, rows) in enumerate(runs):
            r = pl.ds(start, rows)
            copies += [
                pltpu.make_async_copy(dy_hbm.at[r], dy.at[r], row_sem.at[0, b, n]),
                pltpu.make_async_copy(gate_hbm.at[r], gu.at[r, pl.ds(0, f)], row_sem.at[1, b, n]),
                pltpu.make_async_copy(up_hbm.at[r], gu.at[r, pl.ds(f, f)], row_sem.at[2, b, n]),
            ]
        return copies

    def start_rows(b, runs):
        for c in row_copies(b, runs):
            c.start()

    def x_copy(b):
        r = pl.ds(pl.multiple_of(b * BLOCK, BLOCK), BLOCK)
        return pltpu.make_async_copy(x_hbm.at[r], x.at[r], x_sem.at[b])

    first_rows = pl.ds(row_at(2, 0), BLOCK)

    def first_copies(h):
        cols = pl.ds(h * half, half)
        return (
            pltpu.make_async_copy(dy_hbm.at[first_rows, cols], dy.at[first_rows, cols], first_sem.at[0, h]),
            pltpu.make_async_copy(wd_hbm.at[:, cols], wd.at[:, cols], first_sem.at[1, h]),
        )

    def w_copies(n, c):
        r = pl.ds(pl.multiple_of(c * half, half), half)
        return (
            pltpu.make_async_copy(wg_hbm.at[r], w.at[r, pl.ds(0, f)], first_sem.at[2, n]),
            pltpu.make_async_copy(wu_hbm.at[r], w.at[r, pl.ds(f, f)], first_sem.at[3, n]),
        )

    for h in range(2):
        for c in first_copies(h):
            c.start()
    for c in row_copies(0, far_runs(0))[1:]:
        c.start()
    for n, c in enumerate((1 - core, core)):
        for each in w_copies(n, c):
            each.start()
    start_rows(1, far_runs(1))

    def gathered(ref, runs):
        parts = [ref[pl.ds(start, rows), :] for start, rows in runs]
        return parts[0] if len(parts) == 1 else jnp.concatenate(parts, axis=0)

    def offsets(runs):
        return [sum(rows for _, rows in runs[:n]) for n in range(len(runs))]

    def hidden_block(b, runs):
        for c in row_copies(b, runs):
            c.wait()
        dh[: sum(rows for _, rows in runs), :] = dot(gathered(dy, runs), wd[...], (1, 1))
        through_act(runs)

    def through_act(runs):
        for at, (start, rows) in zip(offsets(runs), runs):

            @pl.loop(0, rows // STRIP)
            def _(s):
                here = pl.ds(pl.multiple_of(at + s * STRIP, STRIP), STRIP)
                r = pl.ds(pl.multiple_of(start + s * STRIP, STRIP), STRIP)
                h, back = jax.vjp(act, gu[r, pl.ds(0, f)].astype(jnp.float32), gu[r, pl.ds(f, f)].astype(jnp.float32))
                d_gate, d_up = back(dh[here, :])
                gu[r, pl.ds(0, f)] = d_gate.astype(gu.dtype)
                gu[r, pl.ds(f, f)] = d_up.astype(gu.dtype)
                hid[here, :] = h.astype(hid.dtype)

    def turn_hidden(runs):
        for at, (start, rows) in zip(offsets(runs), runs):
            hid_t[:, pl.ds(pl.multiple_of(start, PART), rows)] = hid[at : at + rows, :].T

    def cols_of(c, q):
        return pl.ds(pl.multiple_of(c * half + q * width, width), width)

    def term_copies(b, runs, q, base=0):
        return [
            remote(
                stage.at[q, pl.ds(base + at, rows)],
                dx.at[pl.ds(start, rows), cols_of(1 - core, q)],
                term_send.at[b, q, n],
                term_recv.at[b, q, n],
                peer,
            )
            for n, (at, (start, rows)) in enumerate(zip(offsets(runs), runs))
        ]

    def stage_free(b, runs):
        for q in range(PIECES):
            for c in term_copies(b, runs, q):
                c.wait_send()

    def term_block(b, runs, base=0):
        n = sum(rows for _, rows in runs)
        for q in range(PIECES):
            stage[q, base : base + n] = dot(gathered(gu, runs), w[cols_of(1 - core, q), :], (1, 1)).astype(stage.dtype)
            for c in term_copies(b, runs, q, base):
                c.start()
        for q in range(PIECES):
            own[q, base : base + n] = dot(gathered(gu, runs), w[cols_of(core, q), :], (1, 1))

    def term_arrived(b, runs, q):
        for c in term_copies(b, runs, q):
            c.wait_recv()

    def summed(at, row, q):
        return own[q, at : at + PART, :] + dx[pl.ds(row, PART), cols_of(core, q)].astype(jnp.float32)

    def far_copy(i, side, q):
        return remote(
            sendbuf.at[i, side, q],
            far.at[side, i, q],
            rs_send.at[i, side, q],
            far_recv.at[side, i, q],
            device_at(steps[side]),
        )

    def near_copy(i, k, side, q):
        b = 2 + 2 * i + k
        return remote(
            sendbuf.at[b, side, q],
            near.at[side, i, k, q],
            rs_send.at[b, side, q],
            near_recv.at[side, i, k, q],
            device_at(steps[side]),
        )

    def first_term(v):
        return remote(
            stage.at[v, pl.ds(0, BLOCK)],
            dx.at[first_rows, cols_of(1 - core, v)],
            first_send.at[v],
            first_recv.at[v],
            peer,
        )

    for h in range(2):
        for c in first_copies(h):
            c.wait()
        part = dot(dy[first_rows, h * half : (h + 1) * half], wd[:, h * half : (h + 1) * half], (1, 1))
        dh[:BLOCK, :] = part if h == 0 else dh[:BLOCK, :] + part
    for c in row_copies(0, far_runs(0))[1:]:
        c.wait()
    through_act(far_runs(0))
    for c in w_copies(0, 1 - core):
        c.wait()
    pl.semaphore_wait(barrier, 3)
    for v in range(PIECES):
        stage[v, :BLOCK] = dot(gu[first_rows, :], w[cols_of(1 - core, v), :], (1, 1)).astype(stage.dtype)
        first_term(v).start()
    for c in w_copies(1, core):
        c.wait()
    for q in range(PIECES):
        own[q, :BLOCK] = dot(gu[first_rows, :], w[cols_of(core, q), :], (1, 1))
    for v in range(PIECES):
        first_term(v).wait_recv()
        for side in range(2):
            sendbuf[0, side, v] = summed(side * PART, row_at(2, 0, side), v).astype(sendbuf.dtype)
            far_copy(0, side, v).start()
    turn_hidden(far_runs(0))
    for k in range(2):
        start_rows(2 + k, sent_runs(0, k))
    x_copy(0).start()

    hidden_block(1, far_runs(1))
    for k in range(2):
        start_rows(4 + k, sent_runs(1, k))
    x_copy(1).start()
    for v in range(PIECES):
        first_term(v).wait_send()
    term_block(1, far_runs(1))
    turn_hidden(far_runs(1))
    for q in range(PIECES):
        term_arrived(1, far_runs(1), q)
        for side in range(2):
            sendbuf[1, side, q] = summed(side * PART, row_at(2, 1, side), q).astype(sendbuf.dtype)
            far_copy(1, side, q).start()

    stage_free(1, far_runs(1))
    start_rows(6, own_runs)

    @pl.loop(0, 2)
    def _(i):
        for n in range(2):
            x_copy(2 + 2 * i + n).start()

        @pl.when(i == 1)
        def _():
            for k in range(2):
                stage_free(2 + k, sent_runs(0, k))

        for k in range(2):
            b, sent = 2 + 2 * i + k, sent_runs(i, k)
            hidden_block(b, sent)
            term_block(b, sent, k * BLOCK)
            turn_hidden(sent)
            for q in range(PIECES):
                term_arrived(b, sent, q)
                for side in range(2):
                    total = summed(k * BLOCK + side * PART, sent[side][0], q)
                    if k == 1:
                        far_copy(i, side, q).wait_recv()
                        total += far[side, i, q].astype(jnp.float32)
                    sendbuf[b, side, q] = total.astype(sendbuf.dtype)
                    near_copy(i, k, side, q).start()

    x_copy(6).start()
    x_copy(7).start()
    hidden_block(6, own_runs)
    for k in range(2):
        stage_free(4 + k, sent_runs(1, k))
    term_block(6, own_runs)
    turn_hidden(own_runs)

    def direct(i, p, side):
        r = pl.ds(row_at(0, i, p), PART)
        return remote(
            dx.at[r, mine], dx.at[r, mine], ag_send.at[side, i, p], ag_recv.at[side, i, p], device_at(steps[side])
        )

    def forward(i, side, k):
        r = pl.ds(pl.multiple_of(row_at(steps[1 - side], i, side) + k * SHARE, SHARE), SHARE)
        return remote(
            dx.at[r, mine], dx.at[r, mine], fwd_send.at[side, i, k], fwd_recv.at[side, i, k], device_at(steps[side])
        )

    peers = []

    def share(step, i, p, rows=PART, k=0):
        n, r = len(peers), pl.ds(pl.multiple_of(row_at(step, i, p) + k * SHARE, SHARE), rows)
        peers.append(remote(dx.at[r, mine], dx.at[r, mine], peer_send.at[n], peer_recv.at[n], peer))
        peers[-1].start()

    def own_block(i):
        for p in range(2):
            for q in range(PIECES):
                total = summed(i * BLOCK + p * PART, row_at(0, i, p), q)
                for side in range(2):
                    k = p if side == 1 else 1 - p
                    near_copy(i, k, side, q).wait_recv()
                    total += near[side, i, k, q].astype(jnp.float32)
                dx[pl.ds(row_at(0, i, p), PART), cols_of(core, q)] = total.astype(dx.dtype)
            direct(i, p, p).start()
        direct(i, 1, 0).start()
        direct(i, 0, 1).start()
        share(0, i, 0, BLOCK)

    def down_tiles(lo, hi):
        @pl.loop(lo, hi)
        def _(t):
            cols = pl.ds(pl.multiple_of(t * (d // 4), d // 4), d // 4)
            dwd[:, cols] = dot(hid_t[...], dy[:, cols], (1, 0)).astype(dwd.dtype)

    def weight_tiles(lo, hi):
        @pl.loop(lo, hi)
        def _(t):
            cols = pl.ds(pl.multiple_of(t * TILE, TILE), TILE)
            dw[cols, :] = dot(x[:, cols], gu[...], (0, 0)).astype(dw.dtype)

    def relay(i):
        for side in range(2):
            direct(i, side, side).wait_recv()
            for k in range(PART // SHARE):
                forward(i, side, k).start()
            share(steps[1 - side], i, side)

    def keep(i):
        for side in range(2):
            direct(i, 1 - side, side).wait_recv()
            share(steps[1 - side], i, 1 - side)

    def last(i):
        for k in range(PART // SHARE):
            for side in range(2):
                forward(i, side, k).wait_recv()
                share(2, i, side, SHARE, k)

    for q in range(PIECES):
        term_arrived(6, own_runs, q)
    own_block(0)
    down_tiles(0, 4)
    for b in range(8):
        x_copy(b).wait()
    weight_tiles(0, 1)
    own_block(1)
    weight_tiles(1, 3)
    relay(0)
    weight_tiles(3, 6)
    keep(0)
    weight_tiles(6, d // TILE)
    relay(1)
    keep(1)

    stage_free(6, own_runs)
    for i in range(2):
        for side in range(2):
            for q in range(PIECES):
                far_copy(i, side, q).wait_send()
                for k in range(2):
                    near_copy(i, k, side, q).wait_send()
            for p in range(2):
                direct(i, p, side).wait_send()
    done = len(peers)
    for c in peers:
        c.wait()
    last(0)
    for side in range(2):
        for k in range(PART // SHARE):
            forward(0, side, k).wait_send()
    last(1)
    for side in range(2):
        for k in range(PART // SHARE):
            forward(1, side, k).wait_send()
    for c in peers[done:]:
        c.wait()


def write_kernel(dx, dw, dwd, dx_hbm, dwg_hbm, dwu_hbm, dwd_hbm, sem):
    f = dwd.shape[0]
    copies = [
        pltpu.make_async_copy(dx, dx_hbm, sem.at[0]),
        pltpu.make_async_copy(dw.at[:, pl.ds(0, f)], dwg_hbm, sem.at[1]),
        pltpu.make_async_copy(dw.at[:, pl.ds(f, f)], dwu_hbm, sem.at[2]),
        pltpu.make_async_copy(dwd, dwd_hbm, sem.at[3]),
    ]
    for c in copies:
        c.start()
    for c in copies:
        c.wait()


def solution(mesh):
    assert mesh.shape["tp"] == 2 * CHIPS

    def step(x, dy, gate, up, w_gate, w_up, w_down):
        tokens, d = x.shape
        f = w_down.shape[0]
        assert tokens == CHIPS * 2 * BLOCK
        half = d // 2
        bf16, f32 = jnp.bfloat16, jnp.float32
        dma = pltpu.SemaphoreType.DMA
        vmem, hbm = pl.BlockSpec(memory_space=pltpu.VMEM), pl.BlockSpec(memory_space=pltpu.HBM)
        dx, dw, dwd = pl.pallas_call(
            main_kernel,
            name="block_grads",
            out_shape=(pltpu.VMEM((tokens, d), bf16), pltpu.VMEM((d, 2 * f), bf16), pltpu.VMEM((f, d), bf16)),
            in_specs=[hbm] * 7,
            out_specs=(vmem,) * 3,
            scratch_shapes=[
                pltpu.VMEM((tokens, d), bf16),
                pltpu.VMEM((tokens, d), bf16),
                pltpu.VMEM((tokens, 2 * f), bf16),
                pltpu.VMEM((d, 2 * f), bf16),
                pltpu.VMEM((f, d), bf16),
                pltpu.VMEM((2 * BLOCK, f), bf16),
                pltpu.VMEM((f, tokens), bf16),
                pltpu.VMEM((2 * BLOCK, f), f32),
                pltpu.VMEM((PIECES, 2 * BLOCK, half // PIECES), f32),
                pltpu.VMEM((PIECES, 2 * BLOCK, half // PIECES), bf16),
                pltpu.VMEM((6, 2, PIECES, PART, half // PIECES), bf16),
                pltpu.VMEM((2, 2, PIECES, PART, half // PIECES), bf16),
                pltpu.VMEM((2, 2, 2, PIECES, PART, half // PIECES), bf16),
                dma((4, 2)),
                dma((3, 7, 2)),
                dma((8,)),
                dma((7, PIECES, 2)),
                dma((7, PIECES, 2)),
                dma((6, 2, PIECES)),
                dma((2, 2, PIECES)),
                dma((2, 2, 2, PIECES)),
                dma((2, 2, 2)),
                dma((2, 2, 2)),
                dma((2, 2, PART // SHARE)),
                dma((2, 2, PART // SHARE)),
                dma((10 + 4 * PART // SHARE,)),
                dma((10 + 4 * PART // SHARE,)),
                dma((PIECES,)),
                dma((PIECES,)),
            ],
            compiler_params=pltpu.CompilerParams(collective_id=0, has_side_effects=True, vmem_limit_bytes=47 * 2**20),
        )(x, dy, gate, up, w_gate, w_up, w_down)
        return pl.pallas_call(
            write_kernel,
            name="write_out",
            out_shape=tuple(
                jax.ShapeDtypeStruct(s, bf16) for s in ((tokens, d), (d, f), (d, f), (f, d))
            ),
            in_specs=[vmem] * 3,
            out_specs=(hbm,) * 4,
            scratch_shapes=[dma((4,))],
            compiler_params=pltpu.CompilerParams(vmem_limit_bytes=20 * 2**20),
        )(dx, dw, dwd)

    tokens, columns, rows = P("dp", None), P(None, "tp"), P("tp", None)
    return jax.shard_map(
        step,
        mesh=mesh,
        in_specs=(tokens, tokens, P("dp", "tp"), P("dp", "tp"), columns, columns, rows),
        out_specs=(tokens, P("dp", "tp"), P("dp", "tp"), P(("dp", "tp"), None)),
        check_vma=False,
    )
```
